32 devices in a mesh: seq: 16 (over z, y, x), dp: 2 (over core).
Axes of the slice: x: 2, y: 2, z: 4, core: 2. Of those that a mesh axis runs over, the one named last changes fastest.
Arguments:
- block_pos: int32 [2, 32], P('dp'), may hold values from 0 to 31, as said below
- queries: bfloat16 [2, 2048, 2048], P('dp', 'seq'), may hold values from -8 to 8
- keys: bfloat16 [2, 2048, 2048], P('dp', 'seq'), may hold values from -4 to 4
- values: bfloat16 [2, 2048, 2048], P('dp', 'seq'), may hold values from -4 to 4
- attn_out: bfloat16 [2, 2048, 2048], P('dp', 'seq'), may hold values from -4 to 4, as said below
- log_sums: float32 [2, 16, 2048], P('dp', None, 'seq'), as said below
- grad_out: bfloat16 [2, 2048, 2048], P('dp', 'seq'), may hold values from -0.375 to 0.375
- out_weight: bfloat16 [2048, 2048], replicated, may hold values from -12 to 12
Outputs:
- grad_queries: bfloat16 [2, 2048, 2048], P('dp', 'seq')
- grad_keys: bfloat16 [2, 2048, 2048], P('dp', 'seq')
- grad_values: bfloat16 [2, 2048, 2048], P('dp', 'seq')
- grad_weight: float32 [2048, 2048], P('seq')
The draws below stay inside these ranges and needn't reach their ends.
Inputs may be any that keep to these rules, and one draw needn't show every extreme that they name: Each row is a permutation of 0 to 31; row block c (rows c * 64 to c * 64 + 63) holds the rows at positions block_pos[b, c] * 64 onward, in order. attn_out is the forward attention output: per head, exp(scores - log_sums) on the allowed keys times values, rounded to bfloat16. log_sums[b, h, t] is the log of the sum of exp(scores[b, h, t, u]) over the keys u with pos[b, u] <= pos[b, t].
All inputs are finite; a program needn't handle non-finite values.
Results may differ from the reference program's by a relative error of at most 0.0075.
Values may be sent and summed in bfloat16 or wider, within the bound.
A program may use at most 320 MiB of HBM per device.

```python
import jax
import jax.numpy as jnp
from jax import lax

HEADS = 16
HEAD_DIM = 128
DW = 2048
TOK_DEV = 128
HD = 2048
BLOCK = 64
GRID = 4
NC = 32
LEN = 2048
SEQS = 2
N_SEQ = 16


def fold_key(base, number):
    return jax.random.fold_in(base, number)


def saved_forward(key):
    base = fold_key(key, 11)
    tables = []
    for index in range(SEQS):
        tables.append(jax.random.permutation(fold_key(base, 100 + index), NC).astype(jnp.int32))
    table_all = jnp.stack(tables)
    width_all = HEADS * HEAD_DIM
    shape = (SEQS, LEN, width_all)
    query_raw = 2.0 * jax.random.truncated_normal(fold_key(base, 1), -4.0, 4.0, shape, jnp.float32)
    key_raw = jax.random.truncated_normal(fold_key(base, 2), -4.0, 4.0, shape, jnp.float32)
    value_raw = jax.random.truncated_normal(fold_key(base, 3), -4.0, 4.0, shape, jnp.float32)
    query_all = query_raw.astype(jnp.bfloat16).astype(jnp.float32)
    key_all = key_raw.astype(jnp.bfloat16).astype(jnp.float32)
    value_all = value_raw.astype(jnp.bfloat16).astype(jnp.float32)
    scaling = HEAD_DIM ** (-0.5)
    outputs = []
    logs = []
    for index in range(SEQS):
        row_index = jnp.arange(LEN, dtype=jnp.int32)
        positions = tables[index][row_index // BLOCK] * BLOCK + row_index % BLOCK
        allowed = positions[None, :] <= positions[:, None]

        def head_forward(pack):
            query_h, key_h, value_h = pack
            scores = jnp.dot(query_h, key_h.T, precision=lax.Precision.HIGHEST) * scaling
            scores = jnp.where(allowed, scores, -1e+30)
            row_max = jnp.max(scores, axis=1)
            log_row = row_max + jnp.log(jnp.sum(jnp.exp(scores - row_max[:, None]), axis=1))
            weights = jnp.exp(scores - log_row[:, None])
            return (jnp.dot(weights, value_h, precision=lax.Precision.HIGHEST), log_row)

        def to_heads(array):
            return jnp.transpose(array.reshape(LEN, HEADS, HEAD_DIM), (1, 0, 2))
        heads_out, heads_log = lax.map(head_forward, (to_heads(query_all[index]), to_heads(key_all[index]), to_heads(value_all[index])))
        outputs.append(jnp.transpose(heads_out, (1, 0, 2)).reshape(LEN, width_all))
        logs.append(heads_log)
    return (table_all, query_all, key_all, value_all, jnp.stack(outputs), jnp.stack(logs))


def draw_block_pos(key, part):
    return saved_forward(key)[0].astype(jnp.int32)


def draw_queries(key, part):
    return saved_forward(key)[1].astype(jnp.bfloat16)


def draw_keys(key, part):
    return saved_forward(key)[2].astype(jnp.bfloat16)


def draw_values(key, part):
    return saved_forward(key)[3].astype(jnp.bfloat16)


def draw_attn_out(key, part):
    return saved_forward(key)[4].astype(jnp.bfloat16)


def draw_log_sums(key, part):
    return saved_forward(key)[5].astype(jnp.float32)


def levels(key, dims, split, low, high):
    def one(axis_at, blocks):
        steps = jax.random.uniform(jax.random.fold_in(jax.random.fold_in(key, 6), axis_at), (blocks,), jnp.float32, low / len(split), high / len(split))
        return jnp.repeat(jnp.exp(steps), dims[axis_at] // blocks).reshape((-1,) + (1,) * (len(dims) - axis_at - 1))

    loudness = one(*split[0])
    for cut in split[1:]:
        loudness = loudness * one(*cut)
    return loudness


def scatter_about(own_key, dims, width, reach, cuts=(), kind=jnp.bfloat16):
    entries = width * jax.random.normal(own_key, dims, jnp.float32)
    if cuts:
        entries = entries * levels(own_key, dims, cuts, -0.22, 0.18)
    return jnp.clip(entries, -reach, reach).astype(kind)


def setup_inputs(seed: int = 0) -> dict:
    seeds = jax.random.split(jax.random.key(seed), 9)
    block_pos = draw_block_pos(jax.random.fold_in(seeds[8], 71), 0)
    queries = draw_queries(jax.random.fold_in(seeds[8], 71), 0)
    keys = draw_keys(jax.random.fold_in(seeds[8], 71), 0)
    values = draw_values(jax.random.fold_in(seeds[8], 71), 0)
    attn_out = draw_attn_out(jax.random.fold_in(seeds[8], 71), 0)
    log_sums = draw_log_sums(jax.random.fold_in(seeds[8], 71), 0)
    grad_out = scatter_about(seeds[6], (SEQS, LEN, DW), 0.0625, 0.375, ((0, 2), (1, 16)))
    out_weight = scatter_about(seeds[7], (HD, DW), 2.0, 12.0)
    return dict(block_pos=block_pos, queries=queries, keys=keys, values=values, attn_out=attn_out, log_sums=log_sums, grad_out=grad_out, out_weight=out_weight)


def run_tables():
    query_owner = jnp.arange(N_SEQ, dtype=jnp.int32)[:, None]
    key_owner = jnp.arange(N_SEQ, dtype=jnp.int32)[None, :]
    distance = (query_owner - key_owner) % N_SEQ
    query_run = (-distance) % GRID
    key_run = ((distance + query_run) // GRID) % GRID
    choose = jnp.arange(GRID, dtype=jnp.int32)
    query_onehot = (query_run[:, :, None] == choose[None, None, :]).astype(jnp.float32)
    key_onehot = (key_run[:, :, None] == choose[None, None, :]).astype(jnp.float32)
    return query_onehot, key_onehot


def grouped_sum(pairs, runs, pattern):
    grouped = jnp.einsum(pattern, pairs, runs, precision=lax.Precision.HIGHEST)
    rounded = lax.optimization_barrier(grouped.astype(jnp.bfloat16))
    return jnp.sum(rounded.astype(jnp.float32), axis=1)


def one_sequence(table_row, query_rows, key_rows, value_rows, saved_out, log_rows, cotangent, out_weight, query_onehot, key_onehot):
    length = query_rows.shape[0]
    width_all = query_rows.shape[1]
    head_count = log_rows.shape[0]
    head_dim = width_all // head_count
    scaling = head_dim ** -0.5
    grad_heads = jnp.dot(cotangent, out_weight.T, preferred_element_type=jnp.float32).astype(jnp.bfloat16)
    deltas = jnp.sum((grad_heads.astype(jnp.float32) * saved_out.astype(jnp.float32)).reshape(length, head_count, head_dim), axis=-1).T
    row_index = jnp.arange(length, dtype=jnp.int32)
    positions = table_row[row_index // BLOCK] * BLOCK + row_index % BLOCK
    allowed = positions[None, :] <= positions[:, None]

    def to_heads(array):
        return jnp.transpose(array.reshape(length, head_count, head_dim), (1, 0, 2))

    def per_head(pack):
        query_h, key_h, value_h, grad_h, log_h, delta_h = pack
        scores = jnp.dot(query_h, key_h.T, preferred_element_type=jnp.float32) * scaling
        attn_probs = jnp.where(allowed, jnp.exp(scores - log_h[:, None]), 0.0)
        probs_low = lax.optimization_barrier(attn_probs.astype(jnp.bfloat16))
        dprobs = jnp.dot(grad_h, value_h.T, preferred_element_type=jnp.float32)
        dscores = attn_probs * (dprobs - delta_h[:, None])
        dscores_low = lax.optimization_barrier(dscores.astype(jnp.bfloat16))
        probs_four = probs_low.astype(jnp.float32).reshape(N_SEQ, TOK_DEV, N_SEQ, TOK_DEV)
        dscore_four = dscores_low.astype(jnp.float32).reshape(N_SEQ, TOK_DEV, N_SEQ, TOK_DEV)
        query_four = query_h.astype(jnp.float32).reshape(N_SEQ, TOK_DEV, head_dim)
        key_four = key_h.astype(jnp.float32).reshape(N_SEQ, TOK_DEV, head_dim)
        grad_four = grad_h.astype(jnp.float32).reshape(N_SEQ, TOK_DEV, head_dim)
        value_pairs = jnp.einsum("iajb,iac->ijbc", probs_four, grad_four, precision=lax.Precision.HIGHEST)
        value_grad = grouped_sum(value_pairs, key_onehot, "ijbc,ijt->jtbc")
        key_pairs = scaling * jnp.einsum("iajb,iac->ijbc", dscore_four, query_four, precision=lax.Precision.HIGHEST)
        key_grad = grouped_sum(key_pairs, key_onehot, "ijbc,ijt->jtbc")
        query_pairs = scaling * jnp.einsum("iajb,jbc->ijac", dscore_four, key_four, precision=lax.Precision.HIGHEST)
        query_grad = grouped_sum(query_pairs, query_onehot, "ijac,ijt->itac")
        return (query_grad.reshape(length, head_dim), key_grad.reshape(length, head_dim), value_grad.reshape(length, head_dim))

    packed = (to_heads(query_rows), to_heads(key_rows), to_heads(value_rows), to_heads(grad_heads), log_rows, deltas)
    query_grad, key_grad, value_grad = lax.map(per_head, packed)

    def from_heads(array):
        return jnp.transpose(array, (1, 0, 2)).reshape(length, width_all).astype(jnp.bfloat16)

    weight_grad = jnp.dot(saved_out.T, cotangent, preferred_element_type=jnp.float32)
    return from_heads(query_grad), from_heads(key_grad), from_heads(value_grad), weight_grad


def reference(block_pos, queries, keys, values, attn_out, log_sums, grad_out, out_weight):
    query_onehot, key_onehot = run_tables()
    query_list = []
    key_list = []
    value_list = []
    weight_total = jnp.zeros(out_weight.shape, jnp.float32)
    for index in range(SEQS):
        outcome = one_sequence(block_pos[index], queries[index], keys[index], values[index], attn_out[index], log_sums[index], grad_out[index], out_weight, query_onehot, key_onehot)
        query_list.append(outcome[0])
        key_list.append(outcome[1])
        value_list.append(outcome[2])
        weight_total = weight_total + outcome[3]
    return (jnp.stack(query_list), jnp.stack(key_list), jnp.stack(value_list), weight_total)
```

```python
import functools

import jax
import jax.numpy as jnp
from jax import lax
from jax.experimental import pallas as pl
from jax.experimental.pallas import tpu as pltpu
from jax.sharding import PartitionSpec as P


def shifted(shard, axis, by):
    count = lax.axis_size(axis)
    return lax.ppermute(shard, axis, [(i, (i + by) % count) for i in range(count)])


def slot_positions(table_row, owners, half_rows):
    slot_ids = owners[:, None] * 2 + jnp.arange(2, dtype=jnp.int32)[None, :]
    pick_rows = (
        slot_ids[:, :, None] == jnp.arange(table_row.shape[0], dtype=jnp.int32)[None, None, :]
    ).astype(jnp.int32)
    block_ids = jnp.sum(pick_rows * table_row[None, None, :], axis=-1)
    offsets = jnp.arange(half_rows, dtype=jnp.int32)
    return (block_ids[:, :, None] * half_rows + offsets[None, None, :]).reshape(
        owners.shape[0], 2 * half_rows
    )


def block_core(
    query_rows, grad_rows, log_block, delta_block, key_rows, value_rows, allowed, scaling
):
    head_count = log_block.shape[0]
    query_len = query_rows.shape[0]
    key_len = key_rows.shape[0]
    query_heads = query_rows.reshape(query_len, head_count, -1)
    grad_split = grad_rows.reshape(query_len, head_count, -1)
    key_heads = key_rows.reshape(key_len, head_count, -1)
    value_heads = value_rows.reshape(key_len, head_count, -1)
    scores = (
        jnp.einsum("ahd,bhd->hab", query_heads, key_heads, preferred_element_type=jnp.float32)
        * scaling
    )
    attn_probs = jnp.where(allowed[None], jnp.exp(scores - log_block[:, :, None]), 0.0)
    probs_low = attn_probs.astype(jnp.bfloat16)
    dprobs = jnp.einsum("ahd,bhd->hab", grad_split, value_heads, preferred_element_type=jnp.float32)
    dscores = attn_probs * (dprobs - delta_block[:, :, None])
    dscores_low = dscores.astype(jnp.bfloat16)
    value_part = jnp.einsum(
        "hab,ahd->bhd", probs_low, grad_split, preferred_element_type=jnp.float32
    )
    key_part = (
        jnp.einsum("hab,ahd->bhd", dscores_low, query_heads, preferred_element_type=jnp.float32)
        * scaling
    )
    query_part = (
        jnp.einsum("hab,bhd->ahd", dscores_low, key_heads, preferred_element_type=jnp.float32)
        * scaling
    )
    return (
        query_part.reshape(query_len, -1),
        key_part.reshape(key_len, -1),
        value_part.reshape(key_len, -1),
    )


def block_grads(
    query_rows, grad_rows, log_block, delta_block, key_rows, value_rows, allowed, scaling
):
    parts = block_core(
        query_rows, grad_rows, log_block, delta_block, key_rows, value_rows, allowed, scaling
    )
    return (parts[0], parts[1].astype(jnp.bfloat16), parts[2].astype(jnp.bfloat16))


def grid_per_device(block_pos, queries, keys, values, attn_out, log_sums, grad_out, out_weight):
    dev_count = lax.axis_size("seq")
    grid_side = 4 + 4 * (dev_count // 64)
    my_index = lax.axis_index("seq")
    table_row = block_pos[0]
    own_queries = queries[0]
    tok_rows = own_queries.shape[0]
    half_rows = tok_rows // 2
    head_count = log_sums.shape[1]
    width_all = own_queries.shape[1]
    scaling = (width_all // head_count) ** (-0.5)
    cotangent = grad_out[0]
    grad_heads = lax.dot_general(
        cotangent, out_weight, (((1,), (1,)), ((), ())), preferred_element_type=jnp.float32
    ).astype(jnp.bfloat16)
    deltas = jnp.einsum(
        "ahd,ahd->ha",
        grad_heads.reshape(tok_rows, head_count, -1),
        attn_out[0].reshape(tok_rows, head_count, -1),
        preferred_element_type=jnp.float32,
    )
    query_pack = (own_queries[None], grad_heads[None], log_sums[0][None], deltas[None])
    key_pack = (keys[0][None], values[0][None])
    query_list = [query_pack]
    key_list = [key_pack]
    for offset in range(1, grid_side):
        query_list.append(
            (
                shifted(query_pack[0].astype(jnp.float32), "seq", offset).astype(jnp.bfloat16),
                shifted(query_pack[1].astype(jnp.float32), "seq", offset).astype(jnp.bfloat16),
                shifted(query_pack[2], "seq", offset),
                shifted(query_pack[3], "seq", offset),
            )
        )
        key_list.append(shifted((key_pack[0], key_pack[1]), "seq", offset * grid_side))
    query_stack = tuple(
        (jnp.concatenate([parcel[member] for parcel in query_list], axis=0) for member in range(4))
    )
    key_stack = tuple(
        (jnp.concatenate([parcel[member] for parcel in key_list], axis=0) for member in range(2))
    )
    query_rows = query_stack[0].reshape(-1, width_all)
    grad_rows = query_stack[1].reshape(-1, width_all)
    log_block = jnp.transpose(query_stack[2], (1, 0, 2)).reshape(head_count, -1)
    delta_block = jnp.transpose(query_stack[3], (1, 0, 2)).reshape(head_count, -1)
    query_owners = (my_index - jnp.arange(grid_side, dtype=jnp.int32)) % dev_count
    key_owners = (my_index - jnp.arange(grid_side, dtype=jnp.int32) * grid_side) % dev_count
    query_pos = slot_positions(table_row, query_owners, half_rows).reshape(-1)
    key_pos = slot_positions(table_row, key_owners, half_rows)
    query_total = jnp.zeros((grid_side * tok_rows, width_all), jnp.float32)
    key_results = []
    for offset in range(grid_side):
        key_now = key_stack[0][offset]
        value_now = key_stack[1][offset]
        allowed = key_pos[offset][None, :] <= query_pos[:, None]
        results = block_grads(
            query_rows, grad_rows, log_block, delta_block, key_now, value_now, allowed, scaling
        )
        query_total = query_total + results[0]
        key_results.append((results[1], results[2]))
    query_parts = query_total.astype(jnp.bfloat16).reshape(grid_side, tok_rows, width_all)
    query_sum = query_parts[0].astype(jnp.float32)
    for offset in range(1, grid_side):
        query_sum = query_sum + shifted(query_parts[offset], "seq", -offset).astype(jnp.float32)
    key_sum = key_results[0][0].astype(jnp.float32)
    value_sum = key_results[0][1].astype(jnp.float32)
    for offset in range(1, grid_side):
        returned = shifted(
            (key_results[offset][0], key_results[offset][1]), "seq", -offset * grid_side
        )
        key_sum = key_sum + returned[0].astype(jnp.float32)
        value_sum = value_sum + returned[1].astype(jnp.float32)
    columns = attn_out[0]
    weight_share = lax.psum_scatter(
        lax.dot_general(
            columns, cotangent, (((0,), (0,)), ((), ())), preferred_element_type=jnp.float32
        ),
        ("seq", "dp"),
        scatter_dimension=0,
        tiled=True,
    )
    weight_share = lax.all_gather(
        weight_share.astype(jnp.bfloat16), "dp", axis=0, tiled=True
    ).astype(weight_share.dtype)
    return (
        query_sum.astype(jnp.bfloat16)[None],
        key_sum.astype(jnp.bfloat16)[None],
        value_sum.astype(jnp.bfloat16)[None],
        weight_share,
    )


MESH = pl.DeviceIdType.MESH
ANY = pl.BlockSpec(memory_space=pl.ANY)


def enter(count, side, cores, me, core, plane):
    barrier = pltpu.get_barrier_semaphore()
    peers = [(lax.rem(me + step, count), core) for step in range(1, count)]
    for turn in range(1, cores):
        peers += [(plane + column, lax.rem(core + turn, cores)) for column in range(side)]
    for peer in peers:
        pl.semaphore_signal(barrier, inc=1, device_id=peer, device_id_type=MESH)
    pl.semaphore_wait(barrier, len(peers))


def fused_kernel(
    count, side, cores, dim, tile, scaling,
    places, q_in, k_in, v_in, a_in, b_in, l_in, w_in,
    q_out, k_out, v_out, w_out,
    q_all, k_all, v_all, g_all, l_all, d_all, a_all, b_all, a_turned,
    a_own, b_own, l_own, w_own, g_own, log_own, delta_own,
    q_row, k_row, v_row, g_row, l_row, d_row, probs_all, dq, dk, dv,
    q_back, k_back, v_back, w_part, w_near, w_mid, w_far, w_half, sources,
    send, recv, a_send, a_recv, b_send, b_recv, pass_send, pass_recv,
    near_send, near_recv, far_send, far_recv,
    back_send, back_recv, half_send, half_recv, local,
):
    me = lax.axis_index("seq")
    core = lax.axis_index("dp")
    column = lax.rem(me, side)
    plane = me - column
    row = me // side
    groups, _, _, sub = w_part.shape
    low = jnp.bfloat16
    near_side = side // 2
    near_base = (row // near_side) * near_side
    near_at = row - near_base
    mirror = side - 1 - row

    loads = [
        pltpu.make_async_copy(source, target, local.at[at])
        for at, (source, target) in enumerate(
            [(l_in, l_own), (b_in, b_own), (w_in, w_own), (a_in, a_own)]
        )
    ]
    for copy in loads:
        copy.start()
    enter(count, side, cores, me, core, plane)

    def head_cut(head):
        return pl.ds(pl.multiple_of(head * dim, dim), dim)

    rows = a_own.shape[0]
    block_rows = rows // 2
    blocks = 2 * count

    def owner_blocks(owner):
        return pl.ds(owner * 2, 2)

    def remote(source, target, sender, receiver, device):
        return pltpu.make_async_remote_copy(
            source, target, sender, receiver, device_id=device, device_id_type=MESH
        )

    def piece(kind, head, owner):
        cut = head_cut(head)
        at = owner_blocks(owner)
        if kind == 0:
            return q_in.at[:, :, cut], q_all.at[at]
        if kind == 1:
            return k_in.at[:, :, cut], k_all.at[at]
        if kind == 2:
            return v_in.at[:, :, cut], v_all.at[at]
        if kind == 3:
            return log_own.at[head], l_all.at[at]
        if kind == 4:
            return g_own.at[head], g_all.at[at]
        return delta_own.at[head], d_all.at[at]

    def outgoing(kind, step):
        peer = lax.rem(me + step, count)
        source, target = piece(kind, peer, me)
        return remote(source, target, send.at[kind, step], recv.at[kind, me], (peer, core))

    def incoming(kind, step):
        peer = lax.rem(me + step, count)
        source, target = piece(kind, me, peer)
        return remote(source, target, send.at[kind, step], recv.at[kind, peer], (peer, core))

    def await_pieces(kinds):
        @pl.loop(1, count)
        def _(step):
            for kind in kinds:
                incoming(kind, step).wait_recv()

    def a_piece(part, to_column, slot):
        return (
            a_in.at[:, head_cut(part * side + to_column)],
            a_all.at[core, slot, :, pl.ds(part * dim, dim)],
        )

    def b_piece(group, to_core, sequence, slot):
        at = pl.ds(pl.multiple_of((to_core * groups + group) * sub, sub), sub)
        return b_in.at[:, at], b_all.at[sequence, slot, :, pl.ds(group * sub, sub)]

    def a_outgoing(part, step):
        to_column = plane_peer(step)
        source, target = a_piece(part, to_column, column)
        return remote(
            source, target, a_send.at[part, step], a_recv.at[part, column],
            (plane + to_column, core),
        )

    def a_incoming(part, step):
        slot = plane_peer(step)
        source, target = a_piece(part, column, slot)
        return remote(
            source, target, a_send.at[part, step], a_recv.at[part, slot], (plane + slot, core)
        )

    def a_pass(sequence, slot, turn):
        block = a_all.at[sequence, slot]
        return remote(
            block, block, pass_send.at[slot, turn], pass_recv.at[slot, sequence],
            (me, lax.rem(core + turn, cores)),
        )

    def b_outgoing(group, step, turn):
        to_column = plane_peer(step)
        to_core = lax.rem(core + turn, cores)
        source, target = b_piece(group, to_core, core, column)
        return remote(
            source, target, b_send.at[group, step, turn], b_recv.at[group, column, core],
            (plane + to_column, to_core),
        )

    def b_incoming(group, step, turn):
        slot = plane_peer(step)
        sequence = lax.rem(core + turn, cores)
        source, target = b_piece(group, core, sequence, slot)
        return remote(
            source, target, b_send.at[group, step, turn], b_recv.at[group, slot, sequence],
            (plane + slot, sequence),
        )

    b_routes = [
        (step, turn) for step in range(side) for turn in range(cores) if step + turn > 0
    ]

    def plane_peer(step):
        return lax.rem(column + step, side)

    def far_first(turn):
        far = count - side
        return jnp.where(turn < far, turn + side, lax.rem(turn - far + 1, side))

    def near_peer(step):
        return near_base + lax.rem(near_at + step, near_side)

    def near_copies(group, to_row, slot, out_index, in_index, device):
        return [
            remote(
                w_part.at[group, part], w_near.at[group, slot, at],
                near_send.at[group, out_index, at], near_recv.at[group, in_index, at], device,
            )
            for at, part in enumerate((to_row, side - 1 - to_row))
        ]

    def far_copy(group):
        return remote(
            w_mid.at[group], w_far.at[group], far_send.at[group], far_recv.at[group],
            (mirror * side + column, core),
        )

    backs = ((q_back, q_out), (k_back, k_out), (v_back, v_out))

    def back_copy(at, owner, head, out_index, in_index, device):
        source, target = backs[at]
        return remote(
            source.at[owner], target.at[:, head_cut(head)],
            back_send.at[at, out_index], back_recv.at[at, in_index], device,
        )

    def start_returns(kinds):
        @pl.loop(0, count - 1)
        def _(turn):
            step = far_first(turn)
            peer = lax.rem(me + step, count)
            for at in kinds:
                back_copy(at, peer, me, step, me, (peer, core)).start()

        for at in kinds:
            source, target = backs[at]
            pltpu.make_async_copy(
                source.at[me], target.at[:, head_cut(me)], local.at[at]
            ).start()

    @pl.loop(0, count - 1)
    def _(turn):
        step = far_first(turn)
        for kind in (0, 1):
            outgoing(kind, step).start()

    for step in range(1, side):
        for part in range(side):
            a_outgoing(part, step).start()
    owns = [
        pltpu.make_async_copy(source, target, local.at[4 + at])
        for at, (source, target) in enumerate(
            [a_piece(part, column, column) for part in range(side)]
            + [b_piece(group, core, core, column) for group in range(groups)]
            + [piece(kind, me, me) for kind in range(3)]
        )
    ]
    for copy in owns:
        copy.start()
    loads[0].wait()
    early_half = lax.broadcasted_iota(jnp.int32, (1, rows), 1) < block_rows
    for head in range(count):
        logs = l_own[head : head + 1, :]
        turned = pltpu.roll(logs, block_rows, 1)
        log_own[head, 0] = jnp.where(early_half, logs, turned)
        log_own[head, 1] = jnp.where(early_half, turned, logs)

    @pl.loop(0, count - 1)
    def _(turn):
        outgoing(3, far_first(turn)).start()

    l_all[owner_blocks(me)] = log_own[me]
    for copy in loads[1:]:
        copy.wait()

    by_rows = (((1,), (1,)), ((), ()))
    by_columns = (((0,), (0,)), ((), ()))

    @pl.loop(0, count)
    def _(turn):
        head = lax.rem(me + far_first(turn), count)
        grads = lax.dot_general(
            b_own[...], w_own[head_cut(head), :], by_rows, preferred_element_type=jnp.float32
        ).astype(low)
        g_own[head] = grads.reshape(2, block_rows, dim)
        product = grads.astype(jnp.float32) * a_own[:, head_cut(head)].astype(jnp.float32)
        deltas = lax.dot_general(
            jnp.ones((8, dim), jnp.float32), product, by_rows,
            precision=lax.Precision.HIGHEST, preferred_element_type=jnp.float32,
        )[0:1]
        turned = pltpu.roll(deltas, block_rows, 1)
        delta_own[head, 0] = jnp.where(early_half, deltas, turned)
        delta_own[head, 1] = jnp.where(early_half, turned, deltas)

        @pl.when(turn > 0)
        def _():
            step = far_first(turn - 1)
            for kind in (4, 5):
                outgoing(kind, step).start()

    g_all[owner_blocks(me)] = g_own[me]
    d_all[owner_blocks(me)] = delta_own[me]

    @pl.loop(0, count - 1)
    def _(turn):
        outgoing(2, far_first(turn)).start()

    for group in range(groups):
        for step, turn in b_routes:
            b_outgoing(group, step, turn).start()

    @pl.loop(0, blocks)
    def _(place):
        found = 0
        for block in range(blocks):
            found = jnp.where(places[0, block] == place, block, found)
        sources[place] = found

    for copy in owns:
        copy.wait()
    def in_order(pairs):
        for place in range(blocks):
            block = sources[place]
            for raw, ordered in pairs:
                ordered[pl.ds(place * block_rows, block_rows), :] = raw[block]

    def in_order_lines(raw, ordered):
        for pair_at in range(blocks // 2):
            early = raw[sources[2 * pair_at]]
            late = raw[sources[2 * pair_at + 1]]
            ordered[pair_at] = jnp.where(early_half, early, late)

    length = count * rows
    tiles = length // tile
    per_tile = tile // rows
    tile_blocks = tile // block_rows
    pairs = tiles * (tiles + 1) // 2

    def pair_of(at):
        j = 0
        for later in range(1, tiles):
            j = j + jnp.where(at >= later * tiles - later * (later - 1) // 2, 1, 0)
        return at - (j * tiles - j * (j - 1) // 2) + j, j

    def cut(at):
        return pl.ds(pl.multiple_of(at * tile, tile), tile)

    def line(ordered, i):
        return jnp.concatenate([ordered[i * per_tile + m] for m in range(per_tile)], axis=1)

    await_pieces((0, 1, 3))
    in_order(((q_all, q_row), (k_all, k_row)))
    in_order_lines(l_all, l_row)

    @pl.loop(0, pairs)
    def _(at):
        i, j = pair_of(at)
        scores = lax.dot_general(
            k_row[cut(j), :], q_row[cut(i), :], by_rows, preferred_element_type=jnp.float32
        )
        key_at = lax.broadcasted_iota(jnp.int32, (tile, tile), 0)
        query_at = lax.broadcasted_iota(jnp.int32, (tile, tile), 1)
        allowed = key_at - query_at <= (i - j) * tile
        probs_all[at] = jnp.where(allowed, jnp.exp(scores * scaling - line(l_row, i)), 0.0)

    rows_all = cores * side * rows

    def weight_stage(group):
        for step, turn in b_routes:
            b_incoming(group, step, turn).wait_recv()
        grads_in = b_all[:, :, :, pl.ds(group * sub, sub)].reshape(rows_all, sub)
        w_part[group] = (
            jnp.dot(a_turned[...], grads_in, preferred_element_type=jnp.float32)
            .astype(low)
            .reshape(side, dim, sub)
        )
        for step in range(1, near_side):
            to_row = near_peer(step)
            device = (to_row * side + column, core)
            for copy in near_copies(group, to_row, near_at, step, near_at, device):
                copy.start()

    def near_sum(group, part, at):
        total = w_part[group, part].astype(jnp.float32)
        for step in range(1, near_side):
            slot = lax.rem(near_at + step, near_side)
            total = total + w_near[group, slot, at].astype(jnp.float32)
        return total

    def cross_stage(group):
        for step in range(1, near_side):
            to_row = near_peer(step)
            device = (to_row * side + column, core)
            for copy in near_copies(group, to_row, near_at, step, near_at, device):
                copy.wait_send()
            slot = to_row - near_base
            for copy in near_copies(group, row, slot, step, slot, device):
                copy.wait_recv()
        w_mid[group] = near_sum(group, mirror, 1).astype(low)
        far_copy(group).start()

    for step in range(side):
        slot = plane_peer(step)
        if step > 0:
            for part in range(side):
                a_incoming(part, step).wait_recv()
        for turn in range(1, cores):
            a_pass(core, slot, turn).start()

    await_pieces((4, 5))
    in_order(((g_all, g_row),))
    in_order_lines(d_all, d_row)
    dv[...] = jnp.zeros_like(dv)
    dk[...] = jnp.zeros_like(dk)
    dq[...] = jnp.zeros_like(dq)

    def add_blocks(total, at, value):
        total[pl.ds(at * tile_blocks, tile_blocks)] += value.reshape(tile_blocks, block_rows, dim)

    @pl.loop(0, pairs)
    def _(at):
        i, j = pair_of(at)
        add_blocks(
            dv, j,
            jnp.dot(probs_all[at].astype(low), g_row[cut(i), :], preferred_element_type=jnp.float32),
        )

    for block in range(blocks):
        target = pl.ds(block % 2 * block_rows, block_rows)
        v_back[block // 2, target, :] = dv[places[0, block]].astype(low)
    start_returns((2,))

    for turn in range(1, cores):
        for slot in range(side):
            a_pass(lax.rem(core + turn, cores), slot, turn).wait_recv()
    for sequence in range(cores):
        for slot in range(side):
            at = pl.ds((sequence * side + slot) * rows, rows)
            a_turned[:, at] = a_all[sequence, slot].T

    await_pieces((2,))
    in_order(((v_all, v_row),))

    @pl.loop(0, pairs)
    def _(at):
        i, j = pair_of(at)
        q_tile, k_tile = q_row[cut(i), :], k_row[cut(j), :]
        dprobs = lax.dot_general(
            v_row[cut(j), :], g_row[cut(i), :], by_rows, preferred_element_type=jnp.float32
        )
        dscores = (probs_all[at] * (dprobs - line(d_row, i))).astype(low)
        add_blocks(dk, j, jnp.dot(dscores, q_tile, preferred_element_type=jnp.float32))
        add_blocks(
            dq, i,
            lax.dot_general(dscores, k_tile, by_columns, preferred_element_type=jnp.float32),
        )

    for block in range(blocks):
        target = pl.ds(block % 2 * block_rows, block_rows)
        k_back[block // 2, target, :] = (dk[places[0, block]] * scaling).astype(low)
    start_returns((1,))
    for block in range(blocks):
        target = pl.ds(block % 2 * block_rows, block_rows)
        q_back[block // 2, target, :] = (dq[places[0, block]] * scaling).astype(low)
    weight_stage(0)
    weight_stage(1)
    start_returns((0,))
    cross_stage(0)
    cross_stage(1)

    for step in range(1, side):
        for part in range(side):
            a_outgoing(part, step).wait_send()
    for turn in range(1, cores):
        for slot in range(side):
            a_pass(core, slot, turn).wait_send()
    for group in range(groups):
        for step, turn in b_routes:
            b_outgoing(group, step, turn).wait_send()

    @pl.loop(1, count)
    def _(step):
        for kind in range(6):
            outgoing(kind, step).wait_send()

    def half_copy(group, slot, turn, other):
        block = w_half.at[group, slot]
        return remote(
            block, block, half_send.at[group, turn], half_recv.at[group, slot], (me, other)
        )

    for group in range(groups):
        far_copy(group).wait_send()
        far_copy(group).wait_recv()
        total = near_sum(group, row, 0) + w_far[group].astype(jnp.float32)
        w_half[group, core] = total.astype(low)
        for turn in range(1, cores):
            half_copy(group, core, turn, lax.rem(core + turn, cores)).start()
    for group in range(groups):
        for turn in range(1, cores):
            other = lax.rem(core + turn, cores)
            half_copy(group, core, turn, other).wait_send()
            half_copy(group, other, turn, other).wait_recv()
        for slot in range(cores):
            w_out[:, pl.ds((slot * groups + group) * sub, sub)] = w_half[group, slot]

    for at, (source, target) in enumerate(backs):
        pltpu.make_async_copy(source.at[me], target.at[:, head_cut(me)], local.at[at]).wait()

    @pl.loop(1, count)
    def _(step):
        peer = lax.rem(me + step, count)
        for at in range(3):
            back_copy(at, peer, me, step, me, (peer, core)).wait_send()
            back_copy(at, me, peer, step, peer, (peer, core)).wait_recv()


def head_per_device(
    side, cores, block_pos, queries, keys, values, attn_out, log_sums, grad_out, out_weight
):
    count = lax.axis_size("seq")
    rows = queries.shape[1]
    width = queries.shape[2]
    heads = log_sums.shape[1]
    dim = width // heads
    scaling = dim ** (-0.5)
    out_width = grad_out.shape[2]
    share = out_width // cores
    length = count * rows
    low = jnp.bfloat16
    block_rows = rows // 2
    groups = 2
    sub = share // groups
    near_side = side // 2
    dma = pltpu.SemaphoreType.DMA
    tile = min(512, length)
    tiles = length // tile
    vmem = pl.BlockSpec(memory_space=pltpu.VMEM)
    wide = (length, dim)
    block_shape = (2 * count, block_rows, dim)
    split = (count, rows, dim)
    lines = (2 * count, 1, rows)
    own_lines = (count, 2, 1, rows)
    grad_queries, grad_keys, grad_values, weight_share = pl.pallas_call(
        functools.partial(fused_kernel, count, side, cores, dim, tile, scaling),
        out_shape=[jax.ShapeDtypeStruct((rows, width), low)] * 3
        + [jax.ShapeDtypeStruct((dim, out_width), low)],
        in_specs=[pl.BlockSpec(memory_space=pltpu.SMEM)] + [ANY] * 7,
        out_specs=[ANY] * 3 + [vmem],
        scratch_shapes=[pltpu.VMEM(block_shape, low)] * 4
        + [pltpu.VMEM(lines, jnp.float32)] * 2
        + [
            pltpu.VMEM((cores, side, rows, side * dim), low),
            pltpu.VMEM((cores, side, rows, share), low),
            pltpu.VMEM((side * dim, cores * side * rows), low),
            pltpu.VMEM((rows, width), low),
            pltpu.VMEM((rows, out_width), low),
            pltpu.VMEM((heads, rows), jnp.float32),
            pltpu.VMEM(out_weight.shape, low),
            pltpu.VMEM((count, 2, block_rows, dim), low),
        ]
        + [pltpu.VMEM(own_lines, jnp.float32)] * 2
        + [pltpu.VMEM(wide, low)] * 4
        + [pltpu.VMEM((count, 1, rows), jnp.float32)] * 2
        + [pltpu.VMEM((tiles * (tiles + 1) // 2, tile, tile), jnp.float32)]
        + [pltpu.VMEM(block_shape, jnp.float32)] * 3
        + [pltpu.VMEM(split, low)] * 3
        + [pltpu.VMEM((groups, side, dim, sub), low)]
        + [pltpu.VMEM((groups, near_side, 2, dim, sub), low)]
        + [pltpu.VMEM((groups, dim, sub), low)] * 2
        + [pltpu.VMEM((groups, cores, dim, sub), low)]
        + [pltpu.SMEM((2 * count,), jnp.int32)]
        + [
            dma((6, count)), dma((6, count)),
            dma((side, side)), dma((side, side)),
            dma((groups, side, cores)), dma((groups, side, cores)),
            dma((side, cores)), dma((side, cores)),
            dma((groups, near_side, 2)), dma((groups, near_side, 2)),
            dma((groups,)), dma((groups,)),
            dma((3, count)), dma((3, count)),
            dma((groups, cores)), dma((groups, cores)), dma((side + groups + 7,)),
        ],
        compiler_params=pltpu.CompilerParams(
            collective_id=0, has_side_effects=True, vmem_limit_bytes=60 * 1024 * 1024
        ),
    )(
        block_pos,
        *(part.reshape(2, block_rows, width) for part in (queries, keys, values)),
        attn_out[0], grad_out[0], log_sums[0],
        out_weight,
    )
    grad_queries, grad_keys, grad_values, weight_share = pl.pallas_call(
        leave_kernel,
        out_shape=[jax.ShapeDtypeStruct((rows, width), low)] * 3
        + [jax.ShapeDtypeStruct((dim, out_width), jnp.float32)],
        in_specs=[vmem] * 4,
        out_specs=[vmem] * 4,
    )(grad_queries, grad_keys, grad_values, weight_share)
    return grad_queries[None], grad_keys[None], grad_values[None], weight_share


def leave_kernel(q_in, k_in, v_in, w_in, q_out, k_out, v_out, w_out):
    for source, target in ((q_in, q_out), (k_in, k_out), (v_in, v_out), (w_in, w_out)):
        target[...] = source[...].astype(target.dtype)


def make_per_device(mesh):
    count = mesh.shape["seq"]
    cores = mesh.shape["dp"]
    side = int(round(count ** 0.5))

    def per_device(block_pos, queries, keys, values, attn_out, log_sums, grad_out, out_weight):
        heads = log_sums.shape[1]
        arguments = (
            block_pos, queries, keys, values, attn_out, log_sums, grad_out, out_weight
        )
        if heads == count and side * side == count and side % 2 == 0:
            return head_per_device(side, cores, *arguments)
        return grid_per_device(*arguments)

    return per_device


def solution(mesh):
    in_specs = (
        P("dp", None),
        P("dp", "seq", None),
        P("dp", "seq", None),
        P("dp", "seq", None),
        P("dp", "seq", None),
        P("dp", None, "seq"),
        P("dp", "seq", None),
        P(),
    )
    out_specs = (P("dp", "seq", None), P("dp", "seq", None), P("dp", "seq", None), P("seq", None))
    return jax.shard_map(
        make_per_device(mesh), mesh=mesh, in_specs=in_specs, out_specs=out_specs, check_vma=False
    )
```

```python
import functools

import jax
import jax.numpy as jnp
from jax import lax
from jax.experimental import pallas as pl
from jax.experimental.pallas import tpu as pltpu
from jax.sharding import PartitionSpec as P


def shifted(shard, axis, by):
    count = lax.axis_size(axis)
    return lax.ppermute(shard, axis, [(i, (i + by) % count) for i in range(count)])


def slot_positions(table_row, owners, half_rows):
    slot_ids = owners[:, None] * 2 + jnp.arange(2, dtype=jnp.int32)[None, :]
    pick_rows = (
        slot_ids[:, :, None] == jnp.arange(table_row.shape[0], dtype=jnp.int32)[None, None, :]
    ).astype(jnp.int32)
    block_ids = jnp.sum(pick_rows * table_row[None, None, :], axis=-1)
    offsets = jnp.arange(half_rows, dtype=jnp.int32)
    return (block_ids[:, :, None] * half_rows + offsets[None, None, :]).reshape(
        owners.shape[0], 2 * half_rows
    )


def block_core(
    query_rows, grad_rows, log_block, delta_block, key_rows, value_rows, allowed, scaling
):
    head_count = log_block.shape[0]
    query_len = query_rows.shape[0]
    key_len = key_rows.shape[0]
    query_heads = query_rows.reshape(query_len, head_count, -1)
    grad_split = grad_rows.reshape(query_len, head_count, -1)
    key_heads = key_rows.reshape(key_len, head_count, -1)
    value_heads = value_rows.reshape(key_len, head_count, -1)
    scores = (
        jnp.einsum("ahd,bhd->hab", query_heads, key_heads, preferred_element_type=jnp.float32)
        * scaling
    )
    attn_probs = jnp.where(allowed[None], jnp.exp(scores - log_block[:, :, None]), 0.0)
    probs_low = attn_probs.astype(jnp.bfloat16)
    dprobs = jnp.einsum("ahd,bhd->hab", grad_split, value_heads, preferred_element_type=jnp.float32)
    dscores = attn_probs * (dprobs - delta_block[:, :, None])
    dscores_low = dscores.astype(jnp.bfloat16)
    value_part = jnp.einsum(
        "hab,ahd->bhd", probs_low, grad_split, preferred_element_type=jnp.float32
    )
    key_part = (
        jnp.einsum("hab,ahd->bhd", dscores_low, query_heads, preferred_element_type=jnp.float32)
        * scaling
    )
    query_part = (
        jnp.einsum("hab,bhd->ahd", dscores_low, key_heads, preferred_element_type=jnp.float32)
        * scaling
    )
    return (
        query_part.reshape(query_len, -1),
        key_part.reshape(key_len, -1),
        value_part.reshape(key_len, -1),
    )


def block_grads(
    query_rows, grad_rows, log_block, delta_block, key_rows, value_rows, allowed, scaling
):
    parts = block_core(
        query_rows, grad_rows, log_block, delta_block, key_rows, value_rows, allowed, scaling
    )
    return (parts[0], parts[1].astype(jnp.bfloat16), parts[2].astype(jnp.bfloat16))


def grid_per_device(block_pos, queries, keys, values, attn_out, log_sums, grad_out, out_weight):
    dev_count = lax.axis_size("seq")
    grid_side = 4 + 4 * (dev_count // 64)
    my_index = lax.axis_index("seq")
    table_row = block_pos[0]
    own_queries = queries[0]
    tok_rows = own_queries.shape[0]
    half_rows = tok_rows // 2
    head_count = log_sums.shape[1]
    width_all = own_queries.shape[1]
    scaling = (width_all // head_count) ** (-0.5)
    cotangent = grad_out[0]
    grad_heads = lax.dot_general(
        cotangent, out_weight, (((1,), (1,)), ((), ())), preferred_element_type=jnp.float32
    ).astype(jnp.bfloat16)
    deltas = jnp.einsum(
        "ahd,ahd->ha",
        grad_heads.reshape(tok_rows, head_count, -1),
        attn_out[0].reshape(tok_rows, head_count, -1),
        preferred_element_type=jnp.float32,
    )
    query_pack = (own_queries[None], grad_heads[None], log_sums[0][None], deltas[None])
    key_pack = (keys[0][None], values[0][None])
    query_list = [query_pack]
    key_list = [key_pack]
    for offset in range(1, grid_side):
        query_list.append(
            (
                shifted(query_pack[0].astype(jnp.float32), "seq", offset).astype(jnp.bfloat16),
                shifted(query_pack[1].astype(jnp.float32), "seq", offset).astype(jnp.bfloat16),
                shifted(query_pack[2], "seq", offset),
                shifted(query_pack[3], "seq", offset),
            )
        )
        key_list.append(shifted((key_pack[0], key_pack[1]), "seq", offset * grid_side))
    query_stack = tuple(
        (jnp.concatenate([parcel[member] for parcel in query_list], axis=0) for member in range(4))
    )
    key_stack = tuple(
        (jnp.concatenate([parcel[member] for parcel in key_list], axis=0) for member in range(2))
    )
    query_rows = query_stack[0].reshape(-1, width_all)
    grad_rows = query_stack[1].reshape(-1, width_all)
    log_block = jnp.transpose(query_stack[2], (1, 0, 2)).reshape(head_count, -1)
    delta_block = jnp.transpose(query_stack[3], (1, 0, 2)).reshape(head_count, -1)
    query_owners = (my_index - jnp.arange(grid_side, dtype=jnp.int32)) % dev_count
    key_owners = (my_index - jnp.arange(grid_side, dtype=jnp.int32) * grid_side) % dev_count
    query_pos = slot_positions(table_row, query_owners, half_rows).reshape(-1)
    key_pos = slot_positions(table_row, key_owners, half_rows)
    query_total = jnp.zeros((grid_side * tok_rows, width_all), jnp.float32)
    key_results = []
    for offset in range(grid_side):
        key_now = key_stack[0][offset]
        value_now = key_stack[1][offset]
        allowed = key_pos[offset][None, :] <= query_pos[:, None]
        results = block_grads(
            query_rows, grad_rows, log_block, delta_block, key_now, value_now, allowed, scaling
        )
        query_total = query_total + results[0]
        key_results.append((results[1], results[2]))
    query_parts = query_total.astype(jnp.bfloat16).reshape(grid_side, tok_rows, width_all)
    query_sum = query_parts[0].astype(jnp.float32)
    for offset in range(1, grid_side):
        query_sum = query_sum + shifted(query_parts[offset], "seq", -offset).astype(jnp.float32)
    key_sum = key_results[0][0].astype(jnp.float32)
    value_sum = key_results[0][1].astype(jnp.float32)
    for offset in range(1, grid_side):
        returned = shifted(
            (key_results[offset][0], key_results[offset][1]), "seq", -offset * grid_side
        )
        key_sum = key_sum + returned[0].astype(jnp.float32)
        value_sum = value_sum + returned[1].astype(jnp.float32)
    columns = attn_out[0]
    weight_share = lax.psum_scatter(
        lax.dot_general(
            columns, cotangent, (((0,), (0,)), ((), ())), preferred_element_type=jnp.float32
        ),
        ("seq", "dp"),
        scatter_dimension=0,
        tiled=True,
    )
    weight_share = lax.all_gather(
        weight_share.astype(jnp.bfloat16), "dp", axis=0, tiled=True
    ).astype(weight_share.dtype)
    return (
        query_sum.astype(jnp.bfloat16)[None],
        key_sum.astype(jnp.bfloat16)[None],
        value_sum.astype(jnp.bfloat16)[None],
        weight_share,
    )


MESH = pl.DeviceIdType.MESH
ANY = pl.BlockSpec(memory_space=pl.ANY)


def enter(count, side, cores, me, core, plane):
    barrier = pltpu.get_barrier_semaphore()
    peers = [(lax.rem(me + step, count), core) for step in range(1, count)]
    for turn in range(1, cores):
        peers += [(plane + column, lax.rem(core + turn, cores)) for column in range(side)]
    for peer in peers:
        pl.semaphore_signal(barrier, inc=1, device_id=peer, device_id_type=MESH)
    pl.semaphore_wait(barrier, len(peers))


def fused_kernel(
    count, side, cores, dim, tile, scaling,
    places, q_in, k_in, v_in, a_in, b_in, l_in, w_in,
    q_out, k_out, v_out, w_out,
    q_all, k_all, v_all, g_all, l_all, d_all, a_all, b_all, a_turned,
    a_own, b_own, l_own, w_own, g_own, log_own, delta_own,
    q_row, k_row, v_row, g_row, l_row, d_row, probs_all, dscores_all, dq, dk, dv,
    q_back, k_back, v_back, w_part, w_near, w_mid, w_far, sources,
    send, recv, a_send, a_recv, b_send, b_recv, pass_send, pass_recv,
    near_send, near_recv, far_send, far_recv,
    back_send, back_recv, half_send, half_recv, local,
):
    me = lax.axis_index("seq")
    core = lax.axis_index("dp")
    column = lax.rem(me, side)
    plane = me - column
    row = me // side
    groups, _, _, sub = w_part.shape
    low = jnp.bfloat16
    near_side = side // 2
    near_base = (row // near_side) * near_side
    near_at = row - near_base
    mirror = side - 1 - row

    loads = [
        pltpu.make_async_copy(source, target, local.at[at])
        for at, (source, target) in enumerate(
            [(l_in, l_own), (b_in, b_own), (w_in, w_own), (a_in, a_own)]
        )
    ]
    for copy in loads:
        copy.start()
    enter(count, side, cores, me, core, plane)

    def head_cut(head):
        return pl.ds(pl.multiple_of(head * dim, dim), dim)

    rows = a_own.shape[0]
    block_rows = rows // 2
    blocks = 2 * count

    def owner_blocks(owner):
        return pl.ds(owner * 2, 2)

    def remote(source, target, sender, receiver, device):
        return pltpu.make_async_remote_copy(
            source, target, sender, receiver, device_id=device, device_id_type=MESH
        )

    def piece(kind, head, owner):
        cut = head_cut(head)
        at = owner_blocks(owner)
        if kind == 0:
            return q_in.at[:, :, cut], q_all.at[at]
        if kind == 1:
            return k_in.at[:, :, cut], k_all.at[at]
        if kind == 2:
            return v_in.at[:, :, cut], v_all.at[at]
        if kind == 3:
            return log_own.at[head], l_all.at[at]
        if kind == 4:
            return g_own.at[head], g_all.at[at]
        return delta_own.at[head], d_all.at[at]

    def outgoing(kind, peer):
        source, target = piece(kind, peer, me)
        return remote(source, target, send.at[kind, peer], recv.at[kind, me], (peer, core))

    def incoming(kind, peer):
        source, target = piece(kind, me, peer)
        return remote(source, target, send.at[kind, peer], recv.at[kind, peer], (peer, core))

    def await_pieces(kinds):
        @pl.loop(0, count - 1)
        def _(turn):
            for kind in kinds:
                incoming(kind, peer_at(turn)).wait_recv()

    def a_piece(part, to_column, slot):
        return (
            a_in.at[:, head_cut(part * side + to_column)],
            a_all.at[core, slot, :, pl.ds(part * dim, dim)],
        )

    def b_piece(group, to_core, sequence, slot):
        at = pl.ds(pl.multiple_of((to_core * groups + group) * sub, sub), sub)
        return b_in.at[:, at], b_all.at[sequence, slot, :, pl.ds(group * sub, sub)]

    def a_outgoing(part, step):
        to_column = plane_peer(step)
        source, target = a_piece(part, to_column, column)
        return remote(
            source, target, a_send.at[part, step], a_recv.at[part, column],
            (plane + to_column, core),
        )

    def a_incoming(part, step):
        slot = plane_peer(step)
        source, target = a_piece(part, column, slot)
        return remote(
            source, target, a_send.at[part, step], a_recv.at[part, slot], (plane + slot, core)
        )

    def a_pass(sequence, slot, turn):
        block = a_all.at[sequence, slot]
        return remote(
            block, block, pass_send.at[slot, turn], pass_recv.at[slot, sequence],
            (me, lax.rem(core + turn, cores)),
        )

    def b_outgoing(group, step, turn):
        to_column = plane_peer(step)
        to_core = lax.rem(core + turn, cores)
        source, target = b_piece(group, to_core, core, column)
        return remote(
            source, target, b_send.at[group, step, turn], b_recv.at[group, column, core],
            (plane + to_column, to_core),
        )

    def b_incoming(group, step, turn):
        slot = plane_peer(step)
        sequence = lax.rem(core + turn, cores)
        source, target = b_piece(group, core, sequence, slot)
        return remote(
            source, target, b_send.at[group, step, turn], b_recv.at[group, slot, sequence],
            (plane + slot, sequence),
        )

    b_routes = [
        (step, turn) for step in range(side) for turn in range(cores) if step + turn > 0
    ]

    def plane_peer(step):
        return lax.rem(column + step, side)

    upward = jnp.where(row < near_side, 1, side - 1)

    def peer_at(turn):
        far = turn < count - side
        next_row = lax.rem(row + (turn // side + 1) * upward, side)
        shift = jnp.where(far, lax.rem(turn, side), turn - (count - side) + 1)
        return jnp.where(far, next_row, row) * side + lax.rem(column + shift, side)

    def near_peer(step):
        return near_base + lax.rem(near_at + step, near_side)

    def near_copies(group, to_row, slot, out_index, in_index, device):
        return [
            remote(
                w_part.at[group, part], w_near.at[group, slot, at],
                near_send.at[group, out_index, at], near_recv.at[group, in_index, at], device,
            )
            for at, part in enumerate((to_row, side - 1 - to_row))
        ]

    def far_copy(group):
        return remote(
            w_mid.at[group], w_far.at[group], far_send.at[group], far_recv.at[group],
            (mirror * side + column, core),
        )

    backs = ((q_back, q_out), (k_back, k_out), (v_back, v_out))

    def back_copy(at, owner, head, out_index, in_index, device):
        source, target = backs[at]
        return remote(
            source.at[owner], target.at[:, head_cut(head)],
            back_send.at[at, out_index], back_recv.at[at, in_index], device,
        )

    def start_returns(kinds):
        @pl.loop(0, count - 1)
        def _(turn):
            peer = peer_at(turn)
            for at in kinds:
                back_copy(at, peer, me, peer, me, (peer, core)).start()

        for at in kinds:
            source, target = backs[at]
            target[:, head_cut(me)] = source[me]

    @pl.loop(0, count - 1)
    def _(turn):
        for kind in (0, 1):
            outgoing(kind, peer_at(turn)).start()

    for step in range(1, side):
        for part in range(side):
            a_outgoing(part, step).start()
    owns = [
        pltpu.make_async_copy(source, target, local.at[4 + at])
        for at, (source, target) in enumerate(
            [a_piece(part, column, column) for part in range(side)]
            + [b_piece(group, core, core, column) for group in range(groups)]
            + [piece(kind, me, me) for kind in range(3)]
        )
    ]
    for copy in owns:
        copy.start()
    loads[0].wait()
    early_half = lax.broadcasted_iota(jnp.int32, (1, rows), 1) < block_rows
    for head in range(count):
        logs = l_own[head : head + 1, :]
        turned = pltpu.roll(logs, block_rows, 1)
        log_own[head, 0] = jnp.where(early_half, logs, turned)
        log_own[head, 1] = jnp.where(early_half, turned, logs)

    @pl.loop(0, count - 1)
    def _(turn):
        outgoing(3, peer_at(turn)).start()

    l_all[owner_blocks(me)] = log_own[me]
    for copy in loads[1:]:
        copy.wait()

    by_rows = (((1,), (1,)), ((), ()))
    by_columns = (((0,), (0,)), ((), ()))

    @pl.loop(0, count)
    def _(turn):
        head = jnp.where(turn < count - 1, peer_at(turn), me)
        grads = lax.dot_general(
            b_own[...], w_own[head_cut(head), :], by_rows, preferred_element_type=jnp.float32
        ).astype(low)
        g_own[head] = grads.reshape(2, block_rows, dim)
        product = grads.astype(jnp.float32) * a_own[:, head_cut(head)].astype(jnp.float32)
        deltas = lax.dot_general(
            jnp.ones((8, dim), jnp.float32), product, by_rows,
            precision=lax.Precision.HIGHEST, preferred_element_type=jnp.float32,
        )[0:1]
        turned = pltpu.roll(deltas, block_rows, 1)
        delta_own[head, 0] = jnp.where(early_half, deltas, turned)
        delta_own[head, 1] = jnp.where(early_half, turned, deltas)

        @pl.when(turn > 0)
        def _():
            for kind in (4, 5):
                outgoing(kind, peer_at(turn - 1)).start()

    g_all[owner_blocks(me)] = g_own[me]
    d_all[owner_blocks(me)] = delta_own[me]

    @pl.loop(0, count - 1)
    def _(turn):
        outgoing(2, peer_at(turn)).start()


    for group in range(groups):
        for step, turn in b_routes:
            b_outgoing(group, step, turn).start()

    @pl.loop(0, blocks)
    def _(place):
        found = 0
        for block in range(blocks):
            found = jnp.where(places[0, block] == place, block, found)
        sources[place] = found

    for copy in owns:
        copy.wait()
    def in_order(pairs):
        for place in range(blocks):
            block = sources[place]
            for raw, ordered in pairs:
                ordered[pl.ds(place * block_rows, block_rows), :] = raw[block]

    def in_order_lines(raw, ordered):
        for pair_at in range(blocks // 2):
            early = raw[sources[2 * pair_at]]
            late = raw[sources[2 * pair_at + 1]]
            ordered[pair_at] = jnp.where(early_half, early, late)

    length = count * rows
    tiles = length // tile
    per_tile = tile // rows
    tile_blocks = tile // block_rows
    pairs = tiles * (tiles + 1) // 2

    def pair_of(at):
        j = 0
        for later in range(1, tiles):
            j = j + jnp.where(at >= later * tiles - later * (later - 1) // 2, 1, 0)
        return at - (j * tiles - j * (j - 1) // 2) + j, j

    def cut(at):
        return pl.ds(pl.multiple_of(at * tile, tile), tile)

    def line(ordered, i):
        return jnp.concatenate([ordered[i * per_tile + m] for m in range(per_tile)], axis=1)

    await_pieces((0, 1, 3))
    in_order(((q_all, q_row), (k_all, k_row)))
    in_order_lines(l_all, l_row)

    @pl.loop(0, pairs)
    def _(at):
        i, j = pair_of(at)
        scores = lax.dot_general(
            k_row[cut(j), :], q_row[cut(i), :], by_rows, preferred_element_type=jnp.float32
        )
        key_at = lax.broadcasted_iota(jnp.int32, (tile, tile), 0)
        query_at = lax.broadcasted_iota(jnp.int32, (tile, tile), 1)
        allowed = key_at - query_at <= (i - j) * tile
        probs_all[at] = jnp.where(allowed, jnp.exp(scores * scaling - line(l_row, i)), 0.0)

    rows_all = cores * side * rows

    def weight_stage(group):
        for step, turn in b_routes:
            b_incoming(group, step, turn).wait_recv()
        grads_in = b_all[:, :, :, pl.ds(group * sub, sub)].reshape(rows_all, sub)
        w_part[group] = (
            jnp.dot(a_turned[...], grads_in, preferred_element_type=jnp.float32)
            .astype(low)
            .reshape(side, dim, sub)
        )
        for step in range(1, near_side):
            to_row = near_peer(step)
            device = (to_row * side + column, core)
            for copy in near_copies(group, to_row, near_at, step, near_at, device):
                copy.start()

    def near_sum(group, part, at):
        total = w_part[group, part].astype(jnp.float32)
        for step in range(1, near_side):
            slot = lax.rem(near_at + step, near_side)
            total = total + w_near[group, slot, at].astype(jnp.float32)
        return total

    def cross_stage(group):
        for step in range(1, near_side):
            to_row = near_peer(step)
            device = (to_row * side + column, core)
            for copy in near_copies(group, to_row, near_at, step, near_at, device):
                copy.wait_send()
            slot = to_row - near_base
            for copy in near_copies(group, row, slot, step, slot, device):
                copy.wait_recv()
        w_mid[group] = near_sum(group, mirror, 1).astype(low)
        far_copy(group).start()

    for step in range(side):
        slot = plane_peer(step)
        if step > 0:
            for part in range(side):
                a_incoming(part, step).wait_recv()
        for turn in range(1, cores):
            a_pass(core, slot, turn).start()

    await_pieces((4, 5))
    in_order(((g_all, g_row),))
    in_order_lines(d_all, d_row)
    dv[...] = jnp.zeros_like(dv)
    dk[...] = jnp.zeros_like(dk)
    dq[...] = jnp.zeros_like(dq)

    def add_blocks(total, at, value):
        total[pl.ds(at * tile_blocks, tile_blocks)] += value.reshape(tile_blocks, block_rows, dim)

    @pl.loop(0, pairs)
    def _(at):
        i, j = pair_of(at)
        add_blocks(
            dv, j,
            jnp.dot(probs_all[at].astype(low), g_row[cut(i), :], preferred_element_type=jnp.float32),
        )

    for block in range(blocks):
        target = pl.ds(block % 2 * block_rows, block_rows)
        v_back[block // 2, target, :] = dv[places[0, block]].astype(low)
    start_returns((2,))

    for turn in range(1, cores):
        for slot in range(side):
            a_pass(lax.rem(core + turn, cores), slot, turn).wait_recv()
    for sequence in range(cores):
        for slot in range(side):
            at = pl.ds((sequence * side + slot) * rows, rows)
            a_turned[:, at] = a_all[sequence, slot].T

    weight_stage(0)
    await_pieces((2,))
    in_order(((v_all, v_row),))

    @pl.loop(0, pairs)
    def _(at):
        i, j = pair_of(at)
        dprobs = lax.dot_general(
            v_row[cut(j), :], g_row[cut(i), :], by_rows, preferred_element_type=jnp.float32
        )
        dscores = (probs_all[at] * (dprobs - line(d_row, i))).astype(low)
        dscores_all[at] = dscores
        add_blocks(dk, j, jnp.dot(dscores, q_row[cut(i), :], preferred_element_type=jnp.float32))

    for block in range(blocks):
        target = pl.ds(block % 2 * block_rows, block_rows)
        k_back[block // 2, target, :] = (dk[places[0, block]] * scaling).astype(low)
    start_returns((1,))
    weight_stage(1)

    @pl.loop(0, pairs)
    def _(at):
        i, j = pair_of(at)
        add_blocks(
            dq, i,
            lax.dot_general(
                dscores_all[at], k_row[cut(j), :], by_columns, preferred_element_type=jnp.float32
            ),
        )

    for block in range(blocks):
        target = pl.ds(block % 2 * block_rows, block_rows)
        q_back[block // 2, target, :] = (dq[places[0, block]] * scaling).astype(low)
    start_returns((0,))
    cross_stage(0)
    cross_stage(1)

    for step in range(1, side):
        for part in range(side):
            a_outgoing(part, step).wait_send()
    for turn in range(1, cores):
        for slot in range(side):
            a_pass(core, slot, turn).wait_send()
    for group in range(groups):
        for step, turn in b_routes:
            b_outgoing(group, step, turn).wait_send()

    @pl.loop(0, count - 1)
    def _(turn):
        for kind in range(6):
            outgoing(kind, peer_at(turn)).wait_send()

    def half_cut(group, slot):
        return pl.ds(pl.multiple_of((slot * groups + group) * sub, sub), sub)

    def half_copy(group, slot, turn, other):
        block = w_out.at[:, half_cut(group, slot)]
        return remote(
            block, block, half_send.at[group, turn], half_recv.at[group, slot], (me, other)
        )

    for group in range(groups):
        far_copy(group).wait_send()
        far_copy(group).wait_recv()
        total = near_sum(group, row, 0) + w_far[group].astype(jnp.float32)
        w_out[:, half_cut(group, core)] = total.astype(low)
        for turn in range(1, cores):
            half_copy(group, core, turn, lax.rem(core + turn, cores)).start()
    for group in range(groups):
        for turn in range(1, cores):
            other = lax.rem(core + turn, cores)
            half_copy(group, core, turn, other).wait_send()
            half_copy(group, other, turn, other).wait_recv()

    @pl.loop(0, count - 1)
    def _(turn):
        peer = peer_at(turn)
        for at in range(3):
            back_copy(at, peer, me, peer, me, (peer, core)).wait_send()
            back_copy(at, me, peer, peer, peer, (peer, core)).wait_recv()


def head_per_device(
    side, cores, block_pos, queries, keys, values, attn_out, log_sums, grad_out, out_weight
):
    count = lax.axis_size("seq")
    rows = queries.shape[1]
    width = queries.shape[2]
    heads = log_sums.shape[1]
    dim = width // heads
    scaling = dim ** (-0.5)
    out_width = grad_out.shape[2]
    share = out_width // cores
    length = count * rows
    low = jnp.bfloat16
    block_rows = rows // 2
    groups = 2
    sub = share // groups
    near_side = side // 2
    dma = pltpu.SemaphoreType.DMA
    tile = min(512, length)
    tiles = length // tile
    vmem = pl.BlockSpec(memory_space=pltpu.VMEM)
    wide = (length, dim)
    block_shape = (2 * count, block_rows, dim)
    split = (count, rows, dim)
    lines = (2 * count, 1, rows)
    own_lines = (count, 2, 1, rows)
    grad_queries, grad_keys, grad_values, weight_share = pl.pallas_call(
        functools.partial(fused_kernel, count, side, cores, dim, tile, scaling),
        out_shape=[pltpu.VMEM((rows, width), low)] * 3 + [pltpu.VMEM((dim, out_width), low)],
        in_specs=[pl.BlockSpec(memory_space=pltpu.SMEM)] + [ANY] * 7,
        out_specs=[vmem] * 4,
        scratch_shapes=[pltpu.VMEM(block_shape, low)] * 4
        + [pltpu.VMEM(lines, jnp.float32)] * 2
        + [
            pltpu.VMEM((cores, side, rows, side * dim), low),
            pltpu.VMEM((cores, side, rows, share), low),
            pltpu.VMEM((side * dim, cores * side * rows), low),
            pltpu.VMEM((rows, width), low),
            pltpu.VMEM((rows, out_width), low),
            pltpu.VMEM((heads, rows), jnp.float32),
            pltpu.VMEM(out_weight.shape, low),
            pltpu.VMEM((count, 2, block_rows, dim), low),
        ]
        + [pltpu.VMEM(own_lines, jnp.float32)] * 2
        + [pltpu.VMEM(wide, low)] * 4
        + [pltpu.VMEM((count, 1, rows), jnp.float32)] * 2
        + [pltpu.VMEM((tiles * (tiles + 1) // 2, tile, tile), kind) for kind in (jnp.float32, low)]
        + [pltpu.VMEM(block_shape, jnp.float32)] * 3
        + [pltpu.VMEM(split, low)] * 3
        + [pltpu.VMEM((groups, side, dim, sub), low)]
        + [pltpu.VMEM((groups, near_side, 2, dim, sub), low)]
        + [pltpu.VMEM((groups, dim, sub), low)] * 2
        + [pltpu.SMEM((2 * count,), jnp.int32)]
        + [
            dma((6, count)), dma((6, count)),
            dma((side, side)), dma((side, side)),
            dma((groups, side, cores)), dma((groups, side, cores)),
            dma((side, cores)), dma((side, cores)),
            dma((groups, near_side, 2)), dma((groups, near_side, 2)),
            dma((groups,)), dma((groups,)),
            dma((3, count)), dma((3, count)),
            dma((groups, cores)), dma((groups, cores)), dma((side + groups + 7,)),
        ],
        compiler_params=pltpu.CompilerParams(
            collective_id=0, has_side_effects=True, vmem_limit_bytes=56 * 1024 * 1024
        ),
    )(
        block_pos,
        *(part.reshape(2, block_rows, width) for part in (queries, keys, values)),
        attn_out[0], grad_out[0], log_sums[0],
        out_weight,
    )
    results = [
        pltpu.with_memory_space_constraint(part, pltpu.VMEM)
        for part in (grad_queries, grad_keys, grad_values, weight_share)
    ]
    grad_queries, grad_keys, grad_values, weight_share = pl.pallas_call(
        leave_kernel,
        out_shape=[jax.ShapeDtypeStruct((rows, width), low)] * 3
        + [jax.ShapeDtypeStruct((dim, out_width), jnp.float32)],
        in_specs=[vmem] * 4,
        out_specs=[ANY] * 4,
        scratch_shapes=[
            pltpu.VMEM((dim, out_width), jnp.float32), pltpu.SemaphoreType.DMA((4,)),
        ],
        compiler_params=pltpu.CompilerParams(vmem_limit_bytes=4 * 1024 * 1024),
    )(*results)
    return grad_queries[None], grad_keys[None], grad_values[None], weight_share


def leave_kernel(q_in, k_in, v_in, w_in, q_out, k_out, v_out, w_out, w_wide, sems):
    copies = [
        pltpu.make_async_copy(source, target, sems.at[at])
        for at, (source, target) in enumerate(
            ((q_in, q_out), (k_in, k_out), (v_in, v_out), (w_wide, w_out))
        )
    ]
    for copy in copies[:3]:
        copy.start()
    w_wide[...] = w_in[...].astype(w_wide.dtype)
    copies[3].start()
    for copy in copies:
        copy.wait()


def make_per_device(mesh):
    count = mesh.shape["seq"]
    cores = mesh.shape["dp"]
    side = int(round(count ** 0.5))

    def per_device(block_pos, queries, keys, values, attn_out, log_sums, grad_out, out_weight):
        heads = log_sums.shape[1]
        arguments = (
            block_pos, queries, keys, values, attn_out, log_sums, grad_out, out_weight
        )
        if heads == count and side * side == count and side % 2 == 0:
            return head_per_device(side, cores, *arguments)
        return grid_per_device(*arguments)

    return per_device


def solution(mesh):
    in_specs = (
        P("dp", None),
        P("dp", "seq", None),
        P("dp", "seq", None),
        P("dp", "seq", None),
        P("dp", "seq", None),
        P("dp", None, "seq"),
        P("dp", "seq", None),
        P(),
    )
    out_specs = (P("dp", "seq", None), P("dp", "seq", None), P("dp", "seq", None), P("seq", None))
    return jax.shard_map(
        make_per_device(mesh), mesh=mesh, in_specs=in_specs, out_specs=out_specs, check_vma=False
    )
```

```python
import functools

import jax
import jax.numpy as jnp
from jax import lax
from jax.experimental import pallas as pl
from jax.experimental.pallas import tpu as pltpu
from jax.sharding import PartitionSpec as P


def shifted(shard, axis, by):
    count = lax.axis_size(axis)
    return lax.ppermute(shard, axis, [(i, (i + by) % count) for i in range(count)])


def slot_positions(table_row, owners, half_rows):
    slot_ids = owners[:, None] * 2 + jnp.arange(2, dtype=jnp.int32)[None, :]
    pick_rows = (
        slot_ids[:, :, None] == jnp.arange(table_row.shape[0], dtype=jnp.int32)[None, None, :]
    ).astype(jnp.int32)
    block_ids = jnp.sum(pick_rows * table_row[None, None, :], axis=-1)
    offsets = jnp.arange(half_rows, dtype=jnp.int32)
    return (block_ids[:, :, None] * half_rows + offsets[None, None, :]).reshape(
        owners.shape[0], 2 * half_rows
    )


def block_core(
    query_rows, grad_rows, log_block, delta_block, key_rows, value_rows, allowed, scaling
):
    head_count = log_block.shape[0]
    query_len = query_rows.shape[0]
    key_len = key_rows.shape[0]
    query_heads = query_rows.reshape(query_len, head_count, -1)
    grad_split = grad_rows.reshape(query_len, head_count, -1)
    key_heads = key_rows.reshape(key_len, head_count, -1)
    value_heads = value_rows.reshape(key_len, head_count, -1)
    scores = (
        jnp.einsum("ahd,bhd->hab", query_heads, key_heads, preferred_element_type=jnp.float32)
        * scaling
    )
    attn_probs = jnp.where(allowed[None], jnp.exp(scores - log_block[:, :, None]), 0.0)
    probs_low = attn_probs.astype(jnp.bfloat16)
    dprobs = jnp.einsum("ahd,bhd->hab", grad_split, value_heads, preferred_element_type=jnp.float32)
    dscores = attn_probs * (dprobs - delta_block[:, :, None])
    dscores_low = dscores.astype(jnp.bfloat16)
    value_part = jnp.einsum(
        "hab,ahd->bhd", probs_low, grad_split, preferred_element_type=jnp.float32
    )
    key_part = (
        jnp.einsum("hab,ahd->bhd", dscores_low, query_heads, preferred_element_type=jnp.float32)
        * scaling
    )
    query_part = (
        jnp.einsum("hab,bhd->ahd", dscores_low, key_heads, preferred_element_type=jnp.float32)
        * scaling
    )
    return (
        query_part.reshape(query_len, -1),
        key_part.reshape(key_len, -1),
        value_part.reshape(key_len, -1),
    )


def block_grads(
    query_rows, grad_rows, log_block, delta_block, key_rows, value_rows, allowed, scaling
):
    parts = block_core(
        query_rows, grad_rows, log_block, delta_block, key_rows, value_rows, allowed, scaling
    )
    return (parts[0], parts[1].astype(jnp.bfloat16), parts[2].astype(jnp.bfloat16))


def grid_per_device(block_pos, queries, keys, values, attn_out, log_sums, grad_out, out_weight):
    dev_count = lax.axis_size("seq")
    grid_side = 4 + 4 * (dev_count // 64)
    my_index = lax.axis_index("seq")
    table_row = block_pos[0]
    own_queries = queries[0]
    tok_rows = own_queries.shape[0]
    half_rows = tok_rows // 2
    head_count = log_sums.shape[1]
    width_all = own_queries.shape[1]
    scaling = (width_all // head_count) ** (-0.5)
    cotangent = grad_out[0]
    grad_heads = lax.dot_general(
        cotangent, out_weight, (((1,), (1,)), ((), ())), preferred_element_type=jnp.float32
    ).astype(jnp.bfloat16)
    deltas = jnp.einsum(
        "ahd,ahd->ha",
        grad_heads.reshape(tok_rows, head_count, -1),
        attn_out[0].reshape(tok_rows, head_count, -1),
        preferred_element_type=jnp.float32,
    )
    query_pack = (own_queries[None], grad_heads[None], log_sums[0][None], deltas[None])
    key_pack = (keys[0][None], values[0][None])
    query_list = [query_pack]
    key_list = [key_pack]
    for offset in range(1, grid_side):
        query_list.append(
            (
                shifted(query_pack[0].astype(jnp.float32), "seq", offset).astype(jnp.bfloat16),
                shifted(query_pack[1].astype(jnp.float32), "seq", offset).astype(jnp.bfloat16),
                shifted(query_pack[2], "seq", offset),
                shifted(query_pack[3], "seq", offset),
            )
        )
        key_list.append(shifted((key_pack[0], key_pack[1]), "seq", offset * grid_side))
    query_stack = tuple(
        (jnp.concatenate([parcel[member] for parcel in query_list], axis=0) for member in range(4))
    )
    key_stack = tuple(
        (jnp.concatenate([parcel[member] for parcel in key_list], axis=0) for member in range(2))
    )
    query_rows = query_stack[0].reshape(-1, width_all)
    grad_rows = query_stack[1].reshape(-1, width_all)
    log_block = jnp.transpose(query_stack[2], (1, 0, 2)).reshape(head_count, -1)
    delta_block = jnp.transpose(query_stack[3], (1, 0, 2)).reshape(head_count, -1)
    query_owners = (my_index - jnp.arange(grid_side, dtype=jnp.int32)) % dev_count
    key_owners = (my_index - jnp.arange(grid_side, dtype=jnp.int32) * grid_side) % dev_count
    query_pos = slot_positions(table_row, query_owners, half_rows).reshape(-1)
    key_pos = slot_positions(table_row, key_owners, half_rows)
    query_total = jnp.zeros((grid_side * tok_rows, width_all), jnp.float32)
    key_results = []
    for offset in range(grid_side):
        key_now = key_stack[0][offset]
        value_now = key_stack[1][offset]
        allowed = key_pos[offset][None, :] <= query_pos[:, None]
        results = block_grads(
            query_rows, grad_rows, log_block, delta_block, key_now, value_now, allowed, scaling
        )
        query_total = query_total + results[0]
        key_results.append((results[1], results[2]))
    query_parts = query_total.astype(jnp.bfloat16).reshape(grid_side, tok_rows, width_all)
    query_sum = query_parts[0].astype(jnp.float32)
    for offset in range(1, grid_side):
        query_sum = query_sum + shifted(query_parts[offset], "seq", -offset).astype(jnp.float32)
    key_sum = key_results[0][0].astype(jnp.float32)
    value_sum = key_results[0][1].astype(jnp.float32)
    for offset in range(1, grid_side):
        returned = shifted(
            (key_results[offset][0], key_results[offset][1]), "seq", -offset * grid_side
        )
        key_sum = key_sum + returned[0].astype(jnp.float32)
        value_sum = value_sum + returned[1].astype(jnp.float32)
    columns = attn_out[0]
    weight_share = lax.psum_scatter(
        lax.dot_general(
            columns, cotangent, (((0,), (0,)), ((), ())), preferred_element_type=jnp.float32
        ),
        ("seq", "dp"),
        scatter_dimension=0,
        tiled=True,
    )
    weight_share = lax.all_gather(
        weight_share.astype(jnp.bfloat16), "dp", axis=0, tiled=True
    ).astype(weight_share.dtype)
    return (
        query_sum.astype(jnp.bfloat16)[None],
        key_sum.astype(jnp.bfloat16)[None],
        value_sum.astype(jnp.bfloat16)[None],
        weight_share,
    )


MESH = pl.DeviceIdType.MESH
ANY = pl.BlockSpec(memory_space=pl.ANY)


def enter(count, side, cores, me, core, plane):
    barrier = pltpu.get_barrier_semaphore()
    peers = [(lax.rem(me + step, count), core) for step in range(1, count)]
    for turn in range(1, cores):
        peers += [(plane + column, lax.rem(core + turn, cores)) for column in range(side)]
    for peer in peers:
        pl.semaphore_signal(barrier, inc=1, device_id=peer, device_id_type=MESH)
    pl.semaphore_wait(barrier, len(peers))


def fused_kernel(
    count, side, cores, dim, tile, scaling,
    places, q_in, k_in, v_in, a_in, b_in, l_in, w_in,
    q_out, k_out, v_out, w_out,
    q_all, k_all, v_all, g_all, l_all, d_all, a_all, b_all, a_turned,
    q_own, k_own, a_own, b_own, l_own, w_own, g_own, log_own, delta_own,
    q_row, k_row, v_row, g_row, l_block, d_block, l_row, d_row, probs_all, dscores_all, dq, dk, dv,
    q_back, k_back, v_back, w_part, w_near, w_mid, w_far, sources,
    send, recv, a_send, a_recv, b_send, b_recv, pass_send, pass_recv,
    near_send, near_recv, far_send, far_recv,
    back_send, back_recv, half_send, half_recv, local,
):
    me = lax.axis_index("seq")
    core = lax.axis_index("dp")
    column = lax.rem(me, side)
    plane = me - column
    row = me // side
    groups, _, _, sub = w_part.shape
    low = jnp.bfloat16
    near_side = side // 2
    near_base = (row // near_side) * near_side
    near_at = row - near_base
    mirror = side - 1 - row

    loads = [
        pltpu.make_async_copy(source, target, local.at[at])
        for at, (source, target) in enumerate(
            [
                (q_in, q_own), (k_in, k_own),
                (l_in, l_own), (b_in, b_own), (w_in, w_own), (a_in, a_own),
            ]
        )
    ]
    for copy in loads:
        copy.start()
    enter(count, side, cores, me, core, plane)

    def head_cut(head):
        return pl.ds(pl.multiple_of(head * dim, dim), dim)

    rows = a_own.shape[0]
    block_rows = rows // 2
    blocks = 2 * count

    def owner_blocks(owner):
        return pl.ds(owner * 2, 2)

    def remote(source, target, sender, receiver, device):
        return pltpu.make_async_remote_copy(
            source, target, sender, receiver, device_id=device, device_id_type=MESH
        )

    def piece(kind, head, owner):
        cut = head_cut(head)
        at = owner_blocks(owner)
        if kind == 0:
            return q_own.at[:, :, cut], q_all.at[at]
        if kind == 1:
            return k_own.at[:, :, cut], k_all.at[at]
        if kind == 2:
            return v_in.at[:, :, cut], v_all.at[at]
        if kind == 3:
            return log_own.at[head], l_all.at[owner]
        if kind == 4:
            return g_own.at[head], g_all.at[at]
        return delta_own.at[head], d_all.at[owner]

    def outgoing(kind, peer):
        source, target = piece(kind, peer, me)
        return remote(source, target, send.at[kind, peer], recv.at[kind, me], (peer, core))

    def incoming(kind, peer):
        source, target = piece(kind, me, peer)
        return remote(source, target, send.at[kind, peer], recv.at[kind, peer], (peer, core))

    def await_pieces(kinds):
        @pl.loop(0, count - 1)
        def _(turn):
            for kind in kinds:
                incoming(kind, peer_at(turn)).wait_recv()

    def a_piece(part, to_column, slot):
        return (
            a_in.at[:, head_cut(part * side + to_column)],
            a_all.at[core, slot, :, pl.ds(part * dim, dim)],
        )

    def b_piece(group, to_core, sequence, slot):
        at = pl.ds(pl.multiple_of((to_core * groups + group) * sub, sub), sub)
        return b_in.at[:, at], b_all.at[sequence, slot, :, pl.ds(group * sub, sub)]

    def a_outgoing(part, step):
        to_column = plane_peer(step)
        source, target = a_piece(part, to_column, column)
        return remote(
            source, target, a_send.at[part, step], a_recv.at[part, column],
            (plane + to_column, core),
        )

    def a_incoming(part, step):
        slot = plane_peer(step)
        source, target = a_piece(part, column, slot)
        return remote(
            source, target, a_send.at[part, step], a_recv.at[part, slot], (plane + slot, core)
        )

    def a_pass(sequence, slot, turn):
        block = a_all.at[sequence, slot]
        return remote(
            block, block, pass_send.at[slot, turn], pass_recv.at[slot, sequence],
            (me, lax.rem(core + turn, cores)),
        )

    def b_outgoing(group, step, turn):
        to_column = plane_peer(step)
        to_core = lax.rem(core + turn, cores)
        source, target = b_piece(group, to_core, core, column)
        return remote(
            source, target, b_send.at[group, step, turn], b_recv.at[group, column, core],
            (plane + to_column, to_core),
        )

    def b_incoming(group, step, turn):
        slot = plane_peer(step)
        sequence = lax.rem(core + turn, cores)
        source, target = b_piece(group, core, sequence, slot)
        return remote(
            source, target, b_send.at[group, step, turn], b_recv.at[group, slot, sequence],
            (plane + slot, sequence),
        )

    b_routes = [
        (step, turn) for step in range(side) for turn in range(cores) if step + turn > 0
    ]

    def plane_peer(step):
        return lax.rem(column + step, side)

    upward = jnp.where(row < near_side, 1, side - 1)

    def peer_at(turn):
        far = turn < count - side
        next_row = lax.rem(row + (turn // side + 1) * upward, side)
        shift = jnp.where(far, lax.rem(turn, side), turn - (count - side) + 1)
        return jnp.where(far, next_row, row) * side + lax.rem(column + shift, side)

    def near_peer(step):
        return near_base + lax.rem(near_at + step, near_side)

    def near_copies(group, to_row, slot, out_index, in_index, device):
        return [
            remote(
                w_part.at[group, part], w_near.at[group, slot, at],
                near_send.at[group, out_index, at], near_recv.at[group, in_index, at], device,
            )
            for at, part in enumerate((to_row, side - 1 - to_row))
        ]

    def far_copy(group):
        return remote(
            w_mid.at[group], w_far.at[group], far_send.at[group], far_recv.at[group],
            (mirror * side + column, core),
        )

    backs = ((q_back, q_out), (k_back, k_out), (v_back, v_out))

    def back_copy(at, owner, head, out_index, in_index, device):
        source, target = backs[at]
        return remote(
            source.at[owner], target.at[:, head_cut(head)],
            back_send.at[at, out_index], back_recv.at[at, in_index], device,
        )

    def start_returns(kinds, first=0, last=count - 1):
        @pl.loop(first, last)
        def _(turn):
            peer = peer_at(turn)
            for at in kinds:
                back_copy(at, peer, me, peer, me, (peer, core)).start()

        if last == count - 1:
            for at in kinds:
                source, target = backs[at]
                target[:, head_cut(me)] = source[me]

    for copy in loads[:2]:
        copy.wait()

    @pl.loop(0, count - 1)
    def _(turn):
        for kind in (0, 1):
            outgoing(kind, peer_at(turn)).start()

    for step in range(1, side):
        for part in range(side):
            a_outgoing(part, step).start()
    owns = [
        pltpu.make_async_copy(source, target, local.at[6 + at])
        for at, (source, target) in enumerate(
            [a_piece(part, column, column) for part in range(side)]
            + [b_piece(group, core, core, column) for group in range(groups)]
            + [piece(2, me, me)]
        )
    ]
    for copy in owns:
        copy.start()
    loads[2].wait()
    early_half = lax.broadcasted_iota(jnp.int32, (1, rows), 1) < block_rows
    for head in range(count):
        log_own[head] = l_own[head : head + 1, :]

    @pl.loop(0, count - 1)
    def _(turn):
        outgoing(3, peer_at(turn)).start()

    q_all[owner_blocks(me)] = q_own[:, :, head_cut(me)]
    k_all[owner_blocks(me)] = k_own[:, :, head_cut(me)]
    l_all[me] = log_own[me]
    for copy in loads[3:]:
        copy.wait()

    by_rows = (((1,), (1,)), ((), ()))
    by_columns = (((0,), (0,)), ((), ()))

    @pl.loop(0, count)
    def _(turn):
        head = jnp.where(turn < count - 1, peer_at(turn), me)
        grads = lax.dot_general(
            b_own[...], w_own[head_cut(head), :], by_rows, preferred_element_type=jnp.float32
        ).astype(low)
        g_own[head] = grads.reshape(2, block_rows, dim)
        product = grads.astype(jnp.float32) * a_own[:, head_cut(head)].astype(jnp.float32)
        deltas = lax.dot_general(
            jnp.ones((8, dim), jnp.float32), product, by_rows,
            precision=lax.Precision.HIGHEST, preferred_element_type=jnp.float32,
        )
        delta_own[head] = deltas[0:1]

        @pl.when(turn > 0)
        def _():
            for kind in (4, 5):
                outgoing(kind, peer_at(turn - 1)).start()

    g_all[owner_blocks(me)] = g_own[me]
    d_all[me] = delta_own[me]

    @pl.loop(0, count - 1)
    def _(turn):
        outgoing(2, peer_at(turn)).start()


    for group in range(groups):
        for step, turn in b_routes:
            b_outgoing(group, step, turn).start()

    @pl.loop(0, blocks)
    def _(place):
        found = 0
        for block in range(blocks):
            found = jnp.where(places[0, block] == place, block, found)
        sources[place] = found

    for copy in owns:
        copy.wait()
    def in_order(pairs):
        for place in range(blocks):
            block = sources[place]
            for raw, ordered in pairs:
                ordered[pl.ds(place * block_rows, block_rows), :] = raw[block]

    def in_order_lines(received, raw, ordered):
        for owner in range(count):
            values = received[owner]
            turned = pltpu.roll(values, block_rows, 1)
            raw[2 * owner] = jnp.where(early_half, values, turned)
            raw[2 * owner + 1] = jnp.where(early_half, turned, values)
        for pair_at in range(blocks // 2):
            early = raw[sources[2 * pair_at]]
            late = raw[sources[2 * pair_at + 1]]
            ordered[pair_at] = jnp.where(early_half, early, late)

    length = count * rows
    tiles = length // tile
    per_tile = tile // rows
    tile_blocks = tile // block_rows
    pairs = tiles * (tiles + 1) // 2

    def pair_of(at):
        j = 0
        for later in range(1, tiles):
            j = j + jnp.where(at >= later * tiles - later * (later - 1) // 2, 1, 0)
        return at - (j * tiles - j * (j - 1) // 2) + j, j

    def cut(at):
        return pl.ds(pl.multiple_of(at * tile, tile), tile)

    def line(ordered, i):
        return jnp.concatenate([ordered[i * per_tile + m] for m in range(per_tile)], axis=1)

    await_pieces((0, 1, 3))
    in_order(((q_all, q_row), (k_all, k_row)))
    in_order_lines(l_all, l_block, l_row)

    @pl.loop(0, pairs)
    def _(at):
        i, j = pair_of(at)
        scores = lax.dot_general(
            k_row[cut(j), :], q_row[cut(i), :], by_rows, preferred_element_type=jnp.float32
        )
        key_at = lax.broadcasted_iota(jnp.int32, (tile, tile), 0)
        query_at = lax.broadcasted_iota(jnp.int32, (tile, tile), 1)
        allowed = key_at - query_at <= (i - j) * tile
        probs_all[at] = jnp.where(allowed, jnp.exp(scores * scaling - line(l_row, i)), 0.0)

    rows_all = cores * side * rows

    def weight_stage(group):
        for step, turn in b_routes:
            b_incoming(group, step, turn).wait_recv()
        grads_in = b_all[:, :, :, pl.ds(group * sub, sub)].reshape(rows_all, sub)
        w_part[group] = (
            jnp.dot(a_turned[...], grads_in, preferred_element_type=jnp.float32)
            .astype(low)
            .reshape(side, dim, sub)
        )
        for step in range(1, near_side):
            to_row = near_peer(step)
            device = (to_row * side + column, core)
            for copy in near_copies(group, to_row, near_at, step, near_at, device):
                copy.start()

    def near_sum(group, part, at):
        total = w_part[group, part].astype(jnp.float32)
        for step in range(1, near_side):
            slot = lax.rem(near_at + step, near_side)
            total = total + w_near[group, slot, at].astype(jnp.float32)
        return total

    def cross_stage(group):
        for step in range(1, near_side):
            to_row = near_peer(step)
            device = (to_row * side + column, core)
            for copy in near_copies(group, to_row, near_at, step, near_at, device):
                copy.wait_send()
            slot = to_row - near_base
            for copy in near_copies(group, row, slot, step, slot, device):
                copy.wait_recv()
        w_mid[group] = near_sum(group, mirror, 1).astype(low)
        far_copy(group).start()

    for step in range(side):
        slot = plane_peer(step)
        if step > 0:
            for part in range(side):
                a_incoming(part, step).wait_recv()
        for turn in range(1, cores):
            a_pass(core, slot, turn).start()

    await_pieces((4, 5))
    in_order(((g_all, g_row),))
    in_order_lines(d_all, d_block, d_row)
    dv[...] = jnp.zeros_like(dv)
    dk[...] = jnp.zeros_like(dk)
    dq[...] = jnp.zeros_like(dq)

    def add_blocks(total, at, value):
        total[pl.ds(at * tile_blocks, tile_blocks)] += value.reshape(tile_blocks, block_rows, dim)

    @pl.loop(0, pairs)
    def _(at):
        i, j = pair_of(at)
        add_blocks(
            dv, j,
            jnp.dot(probs_all[at].astype(low), g_row[cut(i), :], preferred_element_type=jnp.float32),
        )

    for block in range(blocks):
        target = pl.ds(block % 2 * block_rows, block_rows)
        v_back[block // 2, target, :] = dv[places[0, block]].astype(low)
    start_returns((2,))

    for turn in range(1, cores):
        for slot in range(side):
            a_pass(lax.rem(core + turn, cores), slot, turn).wait_recv()
    for sequence in range(cores):
        for slot in range(side):
            at = pl.ds((sequence * side + slot) * rows, rows)
            a_turned[:, at] = a_all[sequence, slot].T

    weight_stage(0)
    await_pieces((2,))
    in_order(((v_all, v_row),))

    @pl.loop(0, pairs)
    def _(at):
        i, j = pair_of(at)
        dprobs = lax.dot_general(
            v_row[cut(j), :], g_row[cut(i), :], by_rows, preferred_element_type=jnp.float32
        )
        dscores = (probs_all[at] * (dprobs - line(d_row, i))).astype(low)
        dscores_all[at] = dscores
        add_blocks(dk, j, jnp.dot(dscores, q_row[cut(i), :], preferred_element_type=jnp.float32))

    for block in range(blocks):
        target = pl.ds(block % 2 * block_rows, block_rows)
        k_back[block // 2, target, :] = (dk[places[0, block]] * scaling).astype(low)
    start_returns((1,))
    weight_stage(1)

    @pl.loop(0, pairs)
    def _(at):
        i, j = pair_of(at)
        add_blocks(
            dq, i,
            lax.dot_general(
                dscores_all[at], k_row[cut(j), :], by_columns, preferred_element_type=jnp.float32
            ),
        )

    for block in range(blocks):
        target = pl.ds(block % 2 * block_rows, block_rows)
        q_back[block // 2, target, :] = (dq[places[0, block]] * scaling).astype(low)
    start_returns((0,))
    cross_stage(0)
    cross_stage(1)

    for step in range(1, side):
        for part in range(side):
            a_outgoing(part, step).wait_send()
    for turn in range(1, cores):
        for slot in range(side):
            a_pass(core, slot, turn).wait_send()
    for group in range(groups):
        for step, turn in b_routes:
            b_outgoing(group, step, turn).wait_send()

    @pl.loop(0, count - 1)
    def _(turn):
        for kind in range(6):
            outgoing(kind, peer_at(turn)).wait_send()

    def half_cut(group, slot):
        return pl.ds(pl.multiple_of((slot * groups + group) * sub, sub), sub)

    def half_copy(group, slot, turn, other):
        block = w_out.at[:, half_cut(group, slot)]
        return remote(
            block, block, half_send.at[group, turn], half_recv.at[group, slot], (me, other)
        )

    for group in range(groups):
        far_copy(group).wait_send()
        far_copy(group).wait_recv()
        total = near_sum(group, row, 0) + w_far[group].astype(jnp.float32)
        w_out[:, half_cut(group, core)] = total.astype(low)
        for turn in range(1, cores):
            half_copy(group, core, turn, lax.rem(core + turn, cores)).start()
    for group in range(groups):
        for turn in range(1, cores):
            other = lax.rem(core + turn, cores)
            half_copy(group, core, turn, other).wait_send()
            half_copy(group, other, turn, other).wait_recv()

    @pl.loop(0, count - 1)
    def _(turn):
        peer = peer_at(turn)
        for at in range(3):
            back_copy(at, peer, me, peer, me, (peer, core)).wait_send()
            back_copy(at, me, peer, peer, peer, (peer, core)).wait_recv()


def head_per_device(
    side, cores, block_pos, queries, keys, values, attn_out, log_sums, grad_out, out_weight
):
    count = lax.axis_size("seq")
    rows = queries.shape[1]
    width = queries.shape[2]
    heads = log_sums.shape[1]
    dim = width // heads
    scaling = dim ** (-0.5)
    out_width = grad_out.shape[2]
    share = out_width // cores
    length = count * rows
    low = jnp.bfloat16
    block_rows = rows // 2
    groups = 2
    sub = share // groups
    near_side = side // 2
    dma = pltpu.SemaphoreType.DMA
    tile = min(512, length)
    tiles = length // tile
    vmem = pl.BlockSpec(memory_space=pltpu.VMEM)
    wide = (length, dim)
    block_shape = (2 * count, block_rows, dim)
    split = (count, rows, dim)
    lines = (2 * count, 1, rows)
    own_lines = (count, 1, rows)
    grad_queries, grad_keys, grad_values, weight_share = pl.pallas_call(
        functools.partial(fused_kernel, count, side, cores, dim, tile, scaling),
        out_shape=[pltpu.VMEM((rows, width), low)] * 3 + [pltpu.VMEM((dim, out_width), low)],
        in_specs=[pl.BlockSpec(memory_space=pltpu.SMEM)] + [ANY] * 7,
        out_specs=[vmem] * 4,
        scratch_shapes=[pltpu.VMEM(block_shape, low)] * 4
        + [pltpu.VMEM(own_lines, jnp.float32)] * 2
        + [
            pltpu.VMEM((cores, side, rows, side * dim), low),
            pltpu.VMEM((cores, side, rows, share), low),
            pltpu.VMEM((side * dim, cores * side * rows), low),
            pltpu.VMEM((2, block_rows, width), low),
            pltpu.VMEM((2, block_rows, width), low),
            pltpu.VMEM((rows, width), low),
            pltpu.VMEM((rows, out_width), low),
            pltpu.VMEM((heads, rows), jnp.float32),
            pltpu.VMEM(out_weight.shape, low),
            pltpu.VMEM((count, 2, block_rows, dim), low),
        ]
        + [pltpu.VMEM(own_lines, jnp.float32)] * 2
        + [pltpu.VMEM(wide, low)] * 4
        + [pltpu.VMEM(lines, jnp.float32)] * 2
        + [pltpu.VMEM(own_lines, jnp.float32)] * 2
        + [pltpu.VMEM((tiles * (tiles + 1) // 2, tile, tile), kind) for kind in (jnp.float32, low)]
        + [pltpu.VMEM(block_shape, jnp.float32)] * 3
        + [pltpu.VMEM(split, low)] * 3
        + [pltpu.VMEM((groups, side, dim, sub), low)]
        + [pltpu.VMEM((groups, near_side, 2, dim, sub), low)]
        + [pltpu.VMEM((groups, dim, sub), low)] * 2
        + [pltpu.SMEM((2 * count,), jnp.int32)]
        + [
            dma((6, count)), dma((6, count)),
            dma((side, side)), dma((side, side)),
            dma((groups, side, cores)), dma((groups, side, cores)),
            dma((side, cores)), dma((side, cores)),
            dma((groups, near_side, 2)), dma((groups, near_side, 2)),
            dma((groups,)), dma((groups,)),
            dma((3, count)), dma((3, count)),
            dma((groups, cores)), dma((groups, cores)), dma((side + groups + 7,)),
        ],
        compiler_params=pltpu.CompilerParams(
            collective_id=0, has_side_effects=True, vmem_limit_bytes=56 * 1024 * 1024
        ),
    )(
        block_pos,
        *(part.reshape(2, block_rows, width) for part in (queries, keys, values)),
        attn_out[0], grad_out[0], log_sums[0],
        out_weight,
    )
    results = [
        pltpu.with_memory_space_constraint(part, pltpu.VMEM)
        for part in (grad_queries, grad_keys, grad_values, weight_share)
    ]
    grad_queries, grad_keys, grad_values, weight_share = pl.pallas_call(
        leave_kernel,
        out_shape=[jax.ShapeDtypeStruct((rows, width), low)] * 3
        + [jax.ShapeDtypeStruct((dim, out_width), jnp.float32)],
        in_specs=[vmem] * 4,
        out_specs=[ANY] * 4,
        scratch_shapes=[
            pltpu.VMEM((dim, out_width), jnp.float32), pltpu.SemaphoreType.DMA((4,)),
        ],
        compiler_params=pltpu.CompilerParams(vmem_limit_bytes=4 * 1024 * 1024),
    )(*results)
    return grad_queries[None], grad_keys[None], grad_values[None], weight_share


def leave_kernel(q_in, k_in, v_in, w_in, q_out, k_out, v_out, w_out, w_wide, sems):
    copies = [
        pltpu.make_async_copy(source, target, sems.at[at])
        for at, (source, target) in enumerate(
            ((q_in, q_out), (k_in, k_out), (v_in, v_out), (w_wide, w_out))
        )
    ]
    for copy in copies[:3]:
        copy.start()
    w_wide[...] = w_in[...].astype(w_wide.dtype)
    copies[3].start()
    for copy in copies:
        copy.wait()


def make_per_device(mesh):
    count = mesh.shape["seq"]
    cores = mesh.shape["dp"]
    side = int(round(count ** 0.5))

    def per_device(block_pos, queries, keys, values, attn_out, log_sums, grad_out, out_weight):
        heads = log_sums.shape[1]
        arguments = (
            block_pos, queries, keys, values, attn_out, log_sums, grad_out, out_weight
        )
        if heads == count and side * side == count and side % 2 == 0:
            return head_per_device(side, cores, *arguments)
        return grid_per_device(*arguments)

    return per_device


def solution(mesh):
    in_specs = (
        P("dp", None),
        P("dp", "seq", None),
        P("dp", "seq", None),
        P("dp", "seq", None),
        P("dp", "seq", None),
        P("dp", None, "seq"),
        P("dp", "seq", None),
        P(),
    )
    out_specs = (P("dp", "seq", None), P("dp", "seq", None), P("dp", "seq", None), P("seq", None))
    return jax.shard_map(
        make_per_device(mesh), mesh=mesh, in_specs=in_specs, out_specs=out_specs, check_vma=False
    )
```

```python
import functools

import jax
import jax.numpy as jnp
from jax import lax
from jax.experimental import pallas as pl
from jax.experimental.pallas import tpu as pltpu
from jax.sharding import PartitionSpec as P


def shifted(shard, axis, by):
    count = lax.axis_size(axis)
    return lax.ppermute(shard, axis, [(i, (i + by) % count) for i in range(count)])


def slot_positions(table_row, owners, half_rows):
    slot_ids = owners[:, None] * 2 + jnp.arange(2, dtype=jnp.int32)[None, :]
    pick_rows = (
        slot_ids[:, :, None] == jnp.arange(table_row.shape[0], dtype=jnp.int32)[None, None, :]
    ).astype(jnp.int32)
    block_ids = jnp.sum(pick_rows * table_row[None, None, :], axis=-1)
    offsets = jnp.arange(half_rows, dtype=jnp.int32)
    return (block_ids[:, :, None] * half_rows + offsets[None, None, :]).reshape(
        owners.shape[0], 2 * half_rows
    )


def block_core(
    query_rows, grad_rows, log_block, delta_block, key_rows, value_rows, allowed, scaling
):
    head_count = log_block.shape[0]
    query_len = query_rows.shape[0]
    key_len = key_rows.shape[0]
    query_heads = query_rows.reshape(query_len, head_count, -1)
    grad_split = grad_rows.reshape(query_len, head_count, -1)
    key_heads = key_rows.reshape(key_len, head_count, -1)
    value_heads = value_rows.reshape(key_len, head_count, -1)
    scores = (
        jnp.einsum("ahd,bhd->hab", query_heads, key_heads, preferred_element_type=jnp.float32)
        * scaling
    )
    attn_probs = jnp.where(allowed[None], jnp.exp(scores - log_block[:, :, None]), 0.0)
    probs_low = attn_probs.astype(jnp.bfloat16)
    dprobs = jnp.einsum("ahd,bhd->hab", grad_split, value_heads, preferred_element_type=jnp.float32)
    dscores = attn_probs * (dprobs - delta_block[:, :, None])
    dscores_low = dscores.astype(jnp.bfloat16)
    value_part = jnp.einsum(
        "hab,ahd->bhd", probs_low, grad_split, preferred_element_type=jnp.float32
    )
    key_part = (
        jnp.einsum("hab,ahd->bhd", dscores_low, query_heads, preferred_element_type=jnp.float32)
        * scaling
    )
    query_part = (
        jnp.einsum("hab,bhd->ahd", dscores_low, key_heads, preferred_element_type=jnp.float32)
        * scaling
    )
    return (
        query_part.reshape(query_len, -1),
        key_part.reshape(key_len, -1),
        value_part.reshape(key_len, -1),
    )


def block_grads(
    query_rows, grad_rows, log_block, delta_block, key_rows, value_rows, allowed, scaling
):
    parts = block_core(
        query_rows, grad_rows, log_block, delta_block, key_rows, value_rows, allowed, scaling
    )
    return (parts[0], parts[1].astype(jnp.bfloat16), parts[2].astype(jnp.bfloat16))


def grid_per_device(block_pos, queries, keys, values, attn_out, log_sums, grad_out, out_weight):
    dev_count = lax.axis_size("seq")
    grid_side = 4 + 4 * (dev_count // 64)
    my_index = lax.axis_index("seq")
    table_row = block_pos[0]
    own_queries = queries[0]
    tok_rows = own_queries.shape[0]
    half_rows = tok_rows // 2
    head_count = log_sums.shape[1]
    width_all = own_queries.shape[1]
    scaling = (width_all // head_count) ** (-0.5)
    cotangent = grad_out[0]
    grad_heads = lax.dot_general(
        cotangent, out_weight, (((1,), (1,)), ((), ())), preferred_element_type=jnp.float32
    ).astype(jnp.bfloat16)
    deltas = jnp.einsum(
        "ahd,ahd->ha",
        grad_heads.reshape(tok_rows, head_count, -1),
        attn_out[0].reshape(tok_rows, head_count, -1),
        preferred_element_type=jnp.float32,
    )
    query_pack = (own_queries[None], grad_heads[None], log_sums[0][None], deltas[None])
    key_pack = (keys[0][None], values[0][None])
    query_list = [query_pack]
    key_list = [key_pack]
    for offset in range(1, grid_side):
        query_list.append(
            (
                shifted(query_pack[0].astype(jnp.float32), "seq", offset).astype(jnp.bfloat16),
                shifted(query_pack[1].astype(jnp.float32), "seq", offset).astype(jnp.bfloat16),
                shifted(query_pack[2], "seq", offset),
                shifted(query_pack[3], "seq", offset),
            )
        )
        key_list.append(shifted((key_pack[0], key_pack[1]), "seq", offset * grid_side))
    query_stack = tuple(
        (jnp.concatenate([parcel[member] for parcel in query_list], axis=0) for member in range(4))
    )
    key_stack = tuple(
        (jnp.concatenate([parcel[member] for parcel in key_list], axis=0) for member in range(2))
    )
    query_rows = query_stack[0].reshape(-1, width_all)
    grad_rows = query_stack[1].reshape(-1, width_all)
    log_block = jnp.transpose(query_stack[2], (1, 0, 2)).reshape(head_count, -1)
    delta_block = jnp.transpose(query_stack[3], (1, 0, 2)).reshape(head_count, -1)
    query_owners = (my_index - jnp.arange(grid_side, dtype=jnp.int32)) % dev_count
    key_owners = (my_index - jnp.arange(grid_side, dtype=jnp.int32) * grid_side) % dev_count
    query_pos = slot_positions(table_row, query_owners, half_rows).reshape(-1)
    key_pos = slot_positions(table_row, key_owners, half_rows)
    query_total = jnp.zeros((grid_side * tok_rows, width_all), jnp.float32)
    key_results = []
    for offset in range(grid_side):
        key_now = key_stack[0][offset]
        value_now = key_stack[1][offset]
        allowed = key_pos[offset][None, :] <= query_pos[:, None]
        results = block_grads(
            query_rows, grad_rows, log_block, delta_block, key_now, value_now, allowed, scaling
        )
        query_total = query_total + results[0]
        key_results.append((results[1], results[2]))
    query_parts = query_total.astype(jnp.bfloat16).reshape(grid_side, tok_rows, width_all)
    query_sum = query_parts[0].astype(jnp.float32)
    for offset in range(1, grid_side):
        query_sum = query_sum + shifted(query_parts[offset], "seq", -offset).astype(jnp.float32)
    key_sum = key_results[0][0].astype(jnp.float32)
    value_sum = key_results[0][1].astype(jnp.float32)
    for offset in range(1, grid_side):
        returned = shifted(
            (key_results[offset][0], key_results[offset][1]), "seq", -offset * grid_side
        )
        key_sum = key_sum + returned[0].astype(jnp.float32)
        value_sum = value_sum + returned[1].astype(jnp.float32)
    columns = attn_out[0]
    weight_share = lax.psum_scatter(
        lax.dot_general(
            columns, cotangent, (((0,), (0,)), ((), ())), preferred_element_type=jnp.float32
        ),
        ("seq", "dp"),
        scatter_dimension=0,
        tiled=True,
    )
    weight_share = lax.all_gather(
        weight_share.astype(jnp.bfloat16), "dp", axis=0, tiled=True
    ).astype(weight_share.dtype)
    return (
        query_sum.astype(jnp.bfloat16)[None],
        key_sum.astype(jnp.bfloat16)[None],
        value_sum.astype(jnp.bfloat16)[None],
        weight_share,
    )


MESH = pl.DeviceIdType.MESH
ANY = pl.BlockSpec(memory_space=pl.ANY)


def enter(count, side, cores, me, core, plane):
    barrier = pltpu.get_barrier_semaphore()
    peers = [(lax.rem(me + step, count), core) for step in range(1, count)]
    for turn in range(1, cores):
        peers += [(plane + column, lax.rem(core + turn, cores)) for column in range(side)]
    for peer in peers:
        pl.semaphore_signal(barrier, inc=1, device_id=peer, device_id_type=MESH)
    pl.semaphore_wait(barrier, len(peers))


def fused_kernel(
    count, side, cores, dim, tile, scaling,
    places, q_in, k_in, v_in, a_in, b_in, l_in, w_in,
    q_out, k_out, v_out, w_out,
    q_all, k_all, v_all, g_all, l_all, d_all, a_all, b_all, a_turned,
    q_own, k_own, a_own, b_own, l_own, w_own, g_own, log_own, delta_own,
    q_row, k_row, v_row, g_row, l_block, d_block, l_row, d_row, probs_all, dscores_all, dq, dk, dv,
    q_back, k_back, v_back, w_part, w_near, w_mid, w_far, sources,
    send, recv, a_send, a_recv, b_send, b_recv, pass_send, pass_recv,
    near_send, near_recv, far_send, far_recv,
    back_send, back_recv, half_send, half_recv, local,
):
    me = lax.axis_index("seq")
    core = lax.axis_index("dp")
    column = lax.rem(me, side)
    plane = me - column
    row = me // side
    groups, _, _, sub = w_part.shape
    low = jnp.bfloat16
    near_side = side // 2
    near_base = (row // near_side) * near_side
    near_at = row - near_base
    mirror = side - 1 - row

    loads = [
        pltpu.make_async_copy(source, target, local.at[at])
        for at, (source, target) in enumerate(
            [
                (q_in, q_own), (k_in, k_own),
                (l_in, l_own), (b_in, b_own), (w_in, w_own), (a_in, a_own),
            ]
        )
    ]
    for copy in loads:
        copy.start()
    enter(count, side, cores, me, core, plane)

    def head_cut(head):
        return pl.ds(pl.multiple_of(head * dim, dim), dim)

    rows = a_own.shape[0]
    block_rows = rows // 2
    blocks = 2 * count

    def owner_blocks(owner):
        return pl.ds(owner * 2, 2)

    def remote(source, target, sender, receiver, device):
        return pltpu.make_async_remote_copy(
            source, target, sender, receiver, device_id=device, device_id_type=MESH
        )

    def piece(kind, head, owner):
        cut = head_cut(head)
        at = owner_blocks(owner)
        if kind == 0:
            return q_own.at[:, :, cut], q_all.at[at]
        if kind == 1:
            return k_own.at[:, :, cut], k_all.at[at]
        if kind == 2:
            return v_in.at[:, :, cut], v_all.at[at]
        if kind == 3:
            return log_own.at[head], l_all.at[owner]
        if kind == 4:
            return g_own.at[head], g_all.at[at]
        return delta_own.at[head], d_all.at[owner]

    def outgoing(kind, peer):
        source, target = piece(kind, peer, me)
        return remote(source, target, send.at[kind, peer], recv.at[kind, me], (peer, core))

    def incoming(kind, peer):
        source, target = piece(kind, me, peer)
        return remote(source, target, send.at[kind, peer], recv.at[kind, peer], (peer, core))

    def await_pieces(kinds):
        @pl.loop(0, count - 1)
        def _(turn):
            for kind in kinds:
                incoming(kind, peer_at(turn)).wait_recv()

    def a_piece(part, to_column, slot):
        return (
            a_in.at[:, head_cut(part * side + to_column)],
            a_all.at[core, slot, :, pl.ds(part * dim, dim)],
        )

    def b_piece(group, to_core, sequence, slot):
        at = pl.ds(pl.multiple_of((to_core * groups + group) * sub, sub), sub)
        return b_in.at[:, at], b_all.at[sequence, slot, :, pl.ds(group * sub, sub)]

    def a_outgoing(part, step):
        to_column = plane_peer(step)
        source, target = a_piece(part, to_column, column)
        return remote(
            source, target, a_send.at[part, step], a_recv.at[part, column],
            (plane + to_column, core),
        )

    def a_incoming(part, step):
        slot = plane_peer(step)
        source, target = a_piece(part, column, slot)
        return remote(
            source, target, a_send.at[part, step], a_recv.at[part, slot], (plane + slot, core)
        )

    def a_pass(sequence, slot, turn):
        block = a_all.at[sequence, slot]
        return remote(
            block, block, pass_send.at[slot, turn], pass_recv.at[slot, sequence],
            (me, lax.rem(core + turn, cores)),
        )

    def b_outgoing(group, step, turn):
        to_column = plane_peer(step)
        to_core = lax.rem(core + turn, cores)
        source, target = b_piece(group, to_core, core, column)
        return remote(
            source, target, b_send.at[group, step, turn], b_recv.at[group, column, core],
            (plane + to_column, to_core),
        )

    def b_incoming(group, step, turn):
        slot = plane_peer(step)
        sequence = lax.rem(core + turn, cores)
        source, target = b_piece(group, core, sequence, slot)
        return remote(
            source, target, b_send.at[group, step, turn], b_recv.at[group, slot, sequence],
            (plane + slot, sequence),
        )

    b_routes = [
        (step, turn) for step in range(side) for turn in range(cores) if step + turn > 0
    ]

    def plane_peer(step):
        return lax.rem(column + step, side)

    upward = jnp.where(row < near_side, 1, side - 1)

    def peer_at(turn):
        far = turn < count - side
        next_row = lax.rem(row + (turn // side + 1) * upward, side)
        shift = jnp.where(far, lax.rem(turn, side), turn - (count - side) + 1)
        return jnp.where(far, next_row, row) * side + lax.rem(column + shift, side)

    def near_peer(step):
        return near_base + lax.rem(near_at + step, near_side)

    def near_copies(group, to_row, slot, out_index, in_index, device):
        return [
            remote(
                w_part.at[group, part], w_near.at[group, slot, at],
                near_send.at[group, out_index, at], near_recv.at[group, in_index, at], device,
            )
            for at, part in enumerate((to_row, side - 1 - to_row))
        ]

    def far_copy(group):
        return remote(
            w_mid.at[group], w_far.at[group], far_send.at[group], far_recv.at[group],
            (mirror * side + column, core),
        )

    backs = ((q_back, q_out), (k_back, k_out), (v_back, v_out))

    def back_copy(at, owner, head, out_index, in_index, device):
        source, target = backs[at]
        return remote(
            source.at[owner], target.at[:, head_cut(head)],
            back_send.at[at, out_index], back_recv.at[at, in_index], device,
        )

    def start_returns(kinds, first=0, last=count - 1):
        @pl.loop(first, last)
        def _(turn):
            peer = peer_at(turn)
            for at in kinds:
                back_copy(at, peer, me, peer, me, (peer, core)).start()

        if last == count - 1:
            for at in kinds:
                source, target = backs[at]
                target[:, head_cut(me)] = source[me]

    for copy in loads[:2]:
        copy.wait()

    @pl.loop(0, count - 1)
    def _(turn):
        for kind in (0, 1):
            outgoing(kind, peer_at(turn)).start()

    for step in range(1, side):
        for part in range(side):
            a_outgoing(part, step).start()
    owns = [
        pltpu.make_async_copy(source, target, local.at[6 + at])
        for at, (source, target) in enumerate(
            [a_piece(part, column, column) for part in range(side)]
            + [b_piece(group, core, core, column) for group in range(groups)]
            + [piece(2, me, me)]
        )
    ]
    for copy in owns:
        copy.start()
    loads[2].wait()
    early_half = lax.broadcasted_iota(jnp.int32, (1, rows), 1) < block_rows
    for head in range(count):
        log_own[head] = l_own[head : head + 1, :]

    @pl.loop(0, count - 1)
    def _(turn):
        outgoing(3, peer_at(turn)).start()

    q_all[owner_blocks(me)] = q_own[:, :, head_cut(me)]
    k_all[owner_blocks(me)] = k_own[:, :, head_cut(me)]
    l_all[me] = log_own[me]
    for copy in loads[3:]:
        copy.wait()

    by_rows = (((1,), (1,)), ((), ()))
    by_columns = (((0,), (0,)), ((), ()))

    @pl.loop(0, count)
    def _(turn):
        head = jnp.where(turn < count - 1, peer_at(turn), me)
        grads = lax.dot_general(
            b_own[...], w_own[head_cut(head), :], by_rows, preferred_element_type=jnp.float32
        ).astype(low)
        g_own[head] = grads.reshape(2, block_rows, dim)
        product = grads.astype(jnp.float32) * a_own[:, head_cut(head)].astype(jnp.float32)
        deltas = lax.dot_general(
            jnp.ones((8, dim), jnp.float32), product, by_rows,
            precision=lax.Precision.HIGHEST, preferred_element_type=jnp.float32,
        )
        delta_own[head] = deltas[0:1]

        @pl.when(turn > 0)
        def _():
            for kind in (4, 5):
                outgoing(kind, peer_at(turn - 1)).start()

    g_all[owner_blocks(me)] = g_own[me]
    d_all[me] = delta_own[me]

    @pl.loop(0, count - 1)
    def _(turn):
        outgoing(2, peer_at(turn)).start()


    for group in range(groups):
        for step, turn in b_routes:
            b_outgoing(group, step, turn).start()

    @pl.loop(0, blocks)
    def _(place):
        found = 0
        for block in range(blocks):
            found = jnp.where(places[0, block] == place, block, found)
        sources[place] = found

    for copy in owns:
        copy.wait()
    def in_order(pairs):
        for place in range(blocks):
            block = sources[place]
            for raw, ordered in pairs:
                ordered[pl.ds(place * block_rows, block_rows), :] = raw[block]

    def in_order_lines(received, raw, ordered):
        for owner in range(count):
            values = received[owner]
            turned = pltpu.roll(values, block_rows, 1)
            raw[2 * owner] = jnp.where(early_half, values, turned)
            raw[2 * owner + 1] = jnp.where(early_half, turned, values)
        for pair_at in range(blocks // 2):
            early = raw[sources[2 * pair_at]]
            late = raw[sources[2 * pair_at + 1]]
            ordered[pair_at] = jnp.where(early_half, early, late)

    length = count * rows
    tiles = length // tile
    per_tile = tile // rows
    tile_blocks = tile // block_rows
    pairs = tiles * (tiles + 1) // 2

    def pair_of(at):
        j = 0
        for later in range(1, tiles):
            j = j + jnp.where(at >= later * tiles - later * (later - 1) // 2, 1, 0)
        return at - (j * tiles - j * (j - 1) // 2) + j, j

    def cut(at):
        return pl.ds(pl.multiple_of(at * tile, tile), tile)

    def line(ordered, i):
        return jnp.concatenate([ordered[i * per_tile + m] for m in range(per_tile)], axis=1)

    await_pieces((0, 1, 3))
    in_order(((q_all, q_row), (k_all, k_row)))
    in_order_lines(l_all, l_block, l_row)

    @pl.loop(0, pairs)
    def _(at):
        i, j = pair_of(at)
        scores = lax.dot_general(
            k_row[cut(j), :], q_row[cut(i), :], by_rows, preferred_element_type=jnp.float32
        )
        key_at = lax.broadcasted_iota(jnp.int32, (tile, tile), 0)
        query_at = lax.broadcasted_iota(jnp.int32, (tile, tile), 1)
        allowed = key_at - query_at <= (i - j) * tile
        probs_all[at] = jnp.where(allowed, jnp.exp(scores * scaling - line(l_row, i)), 0.0)

    rows_all = cores * side * rows

    def weight_stage(group):
        for step, turn in b_routes:
            b_incoming(group, step, turn).wait_recv()
        grads_in = b_all[:, :, :, pl.ds(group * sub, sub)].reshape(rows_all, sub)
        w_part[group] = (
            jnp.dot(a_turned[...], grads_in, preferred_element_type=jnp.float32)
            .astype(low)
            .reshape(side, dim, sub)
        )
        for step in range(1, near_side):
            to_row = near_peer(step)
            device = (to_row * side + column, core)
            for copy in near_copies(group, to_row, near_at, step, near_at, device):
                copy.start()

    def near_sum(group, part, at):
        total = w_part[group, part].astype(jnp.float32)
        for step in range(1, near_side):
            slot = lax.rem(near_at + step, near_side)
            total = total + w_near[group, slot, at].astype(jnp.float32)
        return total

    def cross_stage(group):
        for step in range(1, near_side):
            to_row = near_peer(step)
            device = (to_row * side + column, core)
            for copy in near_copies(group, to_row, near_at, step, near_at, device):
                copy.wait_send()
            slot = to_row - near_base
            for copy in near_copies(group, row, slot, step, slot, device):
                copy.wait_recv()
        w_mid[group] = near_sum(group, mirror, 1).astype(low)
        far_copy(group).start()

    for step in range(side):
        slot = plane_peer(step)
        if step > 0:
            for part in range(side):
                a_incoming(part, step).wait_recv()
        for turn in range(1, cores):
            a_pass(core, slot, turn).start()

    await_pieces((4, 5))
    in_order(((g_all, g_row),))
    in_order_lines(d_all, d_block, d_row)
    dv[...] = jnp.zeros_like(dv)
    dk[...] = jnp.zeros_like(dk)
    dq[...] = jnp.zeros_like(dq)

    def add_blocks(total, at, value):
        total[pl.ds(at * tile_blocks, tile_blocks)] += value.reshape(tile_blocks, block_rows, dim)

    @pl.loop(0, pairs)
    def _(at):
        i, j = pair_of(at)
        add_blocks(
            dv, j,
            jnp.dot(probs_all[at].astype(low), g_row[cut(i), :], preferred_element_type=jnp.float32),
        )

    for block in range(blocks):
        target = pl.ds(block % 2 * block_rows, block_rows)
        v_back[block // 2, target, :] = dv[places[0, block]].astype(low)
    start_returns((2,))

    for turn in range(1, cores):
        for slot in range(side):
            a_pass(lax.rem(core + turn, cores), slot, turn).wait_recv()
    for sequence in range(cores):
        for slot in range(side):
            at = pl.ds((sequence * side + slot) * rows, rows)
            a_turned[:, at] = a_all[sequence, slot].T

    weight_stage(0)
    await_pieces((2,))
    in_order(((v_all, v_row),))

    @pl.loop(0, pairs)
    def _(at):
        i, j = pair_of(at)
        dprobs = lax.dot_general(
            v_row[cut(j), :], g_row[cut(i), :], by_rows, preferred_element_type=jnp.float32
        )
        dscores = (probs_all[at] * (dprobs - line(d_row, i))).astype(low)
        dscores_all[at] = dscores
        add_blocks(dk, j, jnp.dot(dscores, q_row[cut(i), :], preferred_element_type=jnp.float32))

    for block in range(blocks):
        target = pl.ds(block % 2 * block_rows, block_rows)
        k_back[block // 2, target, :] = (dk[places[0, block]] * scaling).astype(low)
    start_returns((1,))
    weight_stage(1)

    @pl.loop(0, pairs)
    def _(at):
        i, j = pair_of(at)
        add_blocks(
            dq, i,
            lax.dot_general(
                dscores_all[at], k_row[cut(j), :], by_columns, preferred_element_type=jnp.float32
            ),
        )

    for block in range(blocks):
        target = pl.ds(block % 2 * block_rows, block_rows)
        q_back[block // 2, target, :] = (dq[places[0, block]] * scaling).astype(low)
    start_returns((0,), 0, count // 2)
    cross_stage(0)
    cross_stage(1)
    start_returns((0,), count // 2)

    for step in range(1, side):
        for part in range(side):
            a_outgoing(part, step).wait_send()
    for turn in range(1, cores):
        for slot in range(side):
            a_pass(core, slot, turn).wait_send()
    for group in range(groups):
        for step, turn in b_routes:
            b_outgoing(group, step, turn).wait_send()

    @pl.loop(0, count - 1)
    def _(turn):
        for kind in range(6):
            outgoing(kind, peer_at(turn)).wait_send()

    def half_cut(group, slot):
        return pl.ds(pl.multiple_of((slot * groups + group) * sub, sub), sub)

    def half_copy(group, slot, turn, other):
        block = w_out.at[:, half_cut(group, slot)]
        return remote(
            block, block, half_send.at[group, turn], half_recv.at[group, slot], (me, other)
        )

    for group in range(groups):
        far_copy(group).wait_send()
        far_copy(group).wait_recv()
        total = near_sum(group, row, 0) + w_far[group].astype(jnp.float32)
        w_out[:, half_cut(group, core)] = total.astype(low)
        for turn in range(1, cores):
            half_copy(group, core, turn, lax.rem(core + turn, cores)).start()
    for group in range(groups):
        for turn in range(1, cores):
            other = lax.rem(core + turn, cores)
            half_copy(group, core, turn, other).wait_send()
            half_copy(group, other, turn, other).wait_recv()

    @pl.loop(0, count - 1)
    def _(turn):
        peer = peer_at(turn)
        for at in range(3):
            back_copy(at, peer, me, peer, me, (peer, core)).wait_send()
            back_copy(at, me, peer, peer, peer, (peer, core)).wait_recv()


def head_per_device(
    side, cores, block_pos, queries, keys, values, attn_out, log_sums, grad_out, out_weight
):
    count = lax.axis_size("seq")
    rows = queries.shape[1]
    width = queries.shape[2]
    heads = log_sums.shape[1]
    dim = width // heads
    scaling = dim ** (-0.5)
    out_width = grad_out.shape[2]
    share = out_width // cores
    length = count * rows
    low = jnp.bfloat16
    block_rows = rows // 2
    groups = 2
    sub = share // groups
    near_side = side // 2
    dma = pltpu.SemaphoreType.DMA
    tile = min(512, length)
    tiles = length // tile
    vmem = pl.BlockSpec(memory_space=pltpu.VMEM)
    wide = (length, dim)
    block_shape = (2 * count, block_rows, dim)
    split = (count, rows, dim)
    lines = (2 * count, 1, rows)
    own_lines = (count, 1, rows)
    grad_queries, grad_keys, grad_values, weight_share = pl.pallas_call(
        functools.partial(fused_kernel, count, side, cores, dim, tile, scaling),
        out_shape=[pltpu.VMEM((rows, width), low)] * 3 + [pltpu.VMEM((dim, out_width), low)],
        in_specs=[pl.BlockSpec(memory_space=pltpu.SMEM)] + [ANY] * 7,
        out_specs=[vmem] * 4,
        scratch_shapes=[pltpu.VMEM(block_shape, low)] * 4
        + [pltpu.VMEM(own_lines, jnp.float32)] * 2
        + [
            pltpu.VMEM((cores, side, rows, side * dim), low),
            pltpu.VMEM((cores, side, rows, share), low),
            pltpu.VMEM((side * dim, cores * side * rows), low),
            pltpu.VMEM((2, block_rows, width), low),
            pltpu.VMEM((2, block_rows, width), low),
            pltpu.VMEM((rows, width), low),
            pltpu.VMEM((rows, out_width), low),
            pltpu.VMEM((heads, rows), jnp.float32),
            pltpu.VMEM(out_weight.shape, low),
            pltpu.VMEM((count, 2, block_rows, dim), low),
        ]
        + [pltpu.VMEM(own_lines, jnp.float32)] * 2
        + [pltpu.VMEM(wide, low)] * 4
        + [pltpu.VMEM(lines, jnp.float32)] * 2
        + [pltpu.VMEM(own_lines, jnp.float32)] * 2
        + [pltpu.VMEM((tiles * (tiles + 1) // 2, tile, tile), kind) for kind in (jnp.float32, low)]
        + [pltpu.VMEM(block_shape, jnp.float32)] * 3
        + [pltpu.VMEM(split, low)] * 3
        + [pltpu.VMEM((groups, side, dim, sub), low)]
        + [pltpu.VMEM((groups, near_side, 2, dim, sub), low)]
        + [pltpu.VMEM((groups, dim, sub), low)] * 2
        + [pltpu.SMEM((2 * count,), jnp.int32)]
        + [
            dma((6, count)), dma((6, count)),
            dma((side, side)), dma((side, side)),
            dma((groups, side, cores)), dma((groups, side, cores)),
            dma((side, cores)), dma((side, cores)),
            dma((groups, near_side, 2)), dma((groups, near_side, 2)),
            dma((groups,)), dma((groups,)),
            dma((3, count)), dma((3, count)),
            dma((groups, cores)), dma((groups, cores)), dma((side + groups + 7,)),
        ],
        compiler_params=pltpu.CompilerParams(
            collective_id=0, has_side_effects=True, vmem_limit_bytes=56 * 1024 * 1024
        ),
    )(
        block_pos,
        *(part.reshape(2, block_rows, width) for part in (queries, keys, values)),
        attn_out[0], grad_out[0], log_sums[0],
        out_weight,
    )
    results = [
        pltpu.with_memory_space_constraint(part, pltpu.VMEM)
        for part in (grad_queries, grad_keys, grad_values, weight_share)
    ]
    grad_queries, grad_keys, grad_values, weight_share = pl.pallas_call(
        leave_kernel,
        out_shape=[jax.ShapeDtypeStruct((rows, width), low)] * 3
        + [jax.ShapeDtypeStruct((dim, out_width), jnp.float32)],
        in_specs=[vmem] * 4,
        out_specs=[ANY] * 4,
        scratch_shapes=[
            pltpu.VMEM((dim, out_width), jnp.float32), pltpu.SemaphoreType.DMA((4,)),
        ],
        compiler_params=pltpu.CompilerParams(vmem_limit_bytes=4 * 1024 * 1024),
    )(*results)
    return grad_queries[None], grad_keys[None], grad_values[None], weight_share


def leave_kernel(q_in, k_in, v_in, w_in, q_out, k_out, v_out, w_out, w_wide, sems):
    copies = [
        pltpu.make_async_copy(source, target, sems.at[at])
        for at, (source, target) in enumerate(
            ((q_in, q_out), (k_in, k_out), (v_in, v_out), (w_wide, w_out))
        )
    ]
    for copy in copies[:3]:
        copy.start()
    w_wide[...] = w_in[...].astype(w_wide.dtype)
    copies[3].start()
    for copy in copies:
        copy.wait()


def make_per_device(mesh):
    count = mesh.shape["seq"]
    cores = mesh.shape["dp"]
    side = int(round(count ** 0.5))

    def per_device(block_pos, queries, keys, values, attn_out, log_sums, grad_out, out_weight):
        heads = log_sums.shape[1]
        arguments = (
            block_pos, queries, keys, values, attn_out, log_sums, grad_out, out_weight
        )
        if heads == count and side * side == count and side % 2 == 0:
            return head_per_device(side, cores, *arguments)
        return grid_per_device(*arguments)

    return per_device


def solution(mesh):
    in_specs = (
        P("dp", None),
        P("dp", "seq", None),
        P("dp", "seq", None),
        P("dp", "seq", None),
        P("dp", "seq", None),
        P("dp", None, "seq"),
        P("dp", "seq", None),
        P(),
    )
    out_specs = (P("dp", "seq", None), P("dp", "seq", None), P("dp", "seq", None), P("seq", None))
    return jax.shard_map(
        make_per_device(mesh), mesh=mesh, in_specs=in_specs, out_specs=out_specs, check_vma=False
    )
```
